32 devices in a mesh: groups: 2 (over x), gx: 16 (over z, y, core).
Axes of the slice: x: 2, y: 2, z: 4, core: 2. Of those that a mesh axis runs over, the one named last changes fastest.
Arguments:
- volume: bfloat16 [32, 64, 16, 256], P(None, ('groups', 'gx')), parts along dimension 1, may hold values from -6 to 6
- weight_two: bfloat16 [32, 32, 3, 3, 3], replicated, may hold values from -0.21875 to 0.21875
- weight_three: bfloat16 [64, 32, 3, 3, 3], replicated, may hold values from -0.21875 to 0.21875
- cotangent: bfloat16 [64, 32, 8, 128], P(None, ('groups', 'gx')), parts along dimension 1, may hold values from -6 to 6
Outputs:
- features_three: bfloat16 [64, 32, 8, 128], P(None, ('groups', 'gx')), parts along dimension 1
- grad_three: float32 [128, 32, 3, 3, 3], P(('groups', 'gx')), parts along dimension 0
- grad_two: float32 [64, 32, 3, 3, 3], P('groups'), parts along dimension 0
- grad_volume: bfloat16 [32, 64, 16, 256], P(None, ('groups', 'gx')), parts along dimension 1
The draws below stay inside these ranges and needn't reach their ends.
There are 2 independent parts, one for each index of `groups`. The reference program is written for one: setup_inputs(seed, part) draws one part's arguments, and reference() takes and returns one part's arrays. A program takes and returns all parts, laid end to end along the dimension named above; an argument that names none is the same for every part. Nothing has to cross between parts.
All inputs are finite; a program needn't handle non-finite values.
Results may differ from the reference program's by a relative error of at most 0.012.
Values may be sent and summed in bfloat16 or wider, within the bound.
No kernel may reach another device: no remote copies, remote signals or barrier semaphores. Data moves between devices by JAX's collectives and lax.ppermute only.
A program may use at most 128 MiB of HBM per device.

```python
import jax
import jax.numpy as jnp
from jax import lax

CHANNELS = 32
FILTERS = 64
HEIGHT = 16
WIDTH = 256
DEPTH = 32
DEPTH_HALF = 16
HEIGHT_HALF = 8
WIDTH_HALF = 128


def spiked(array, stream_key, source, target, blocks, factor):
    def block_of(position):
        return (jnp.arange(array.shape[position]) // (array.shape[position] // blocks)).reshape((-1,) + (1,) * (array.ndim - 1 - position))

    first = jax.random.permutation(stream_key, blocks)[block_of(target)]
    far = (block_of(target) + blocks // 2) % blocks
    return jnp.where((block_of(source) == first) | (block_of(source) == far), factor * array, array)


def block_levels(rng, shape, shards, least, largest):
    factor_of, own = 1.0, jax.random.fold_in(rng, 6)
    for dim, shards_of in shards:
        steps = jnp.exp(jax.random.uniform(jax.random.fold_in(own, dim), (shards_of,), jnp.float32, least / len(shards), largest / len(shards)))
        factor_of = factor_of * jnp.repeat(steps, shape[dim] // shards_of).reshape([-1 if axis == dim else 1 for axis in range(len(shape))])
    return factor_of


def noise(rng, extent, deviation, limit, pieces=(), held_as=jnp.bfloat16):
    values = jax.random.normal(rng, extent, jnp.float32) * deviation
    if len(pieces) > 0:
        values = block_levels(rng, extent, pieces, -0.22, 0.18) * values
    return jnp.clip(values, min=-limit, max=limit).astype(held_as)


def gaussian_with(stream_key, dims, scale, bound, shards, heavy, kind=jnp.bfloat16):
    values = scale * jax.random.normal(stream_key, dims, jnp.float32)
    if shards:
        values = values * block_levels(stream_key, dims, shards, -0.22, 0.18)
    return jnp.clip(spiked(values, jax.random.fold_in(stream_key, 3), *heavy), -bound, bound).astype(kind)


def setup_inputs(seed: int = 0, part: int = 0) -> dict:
    keys = jax.random.split(jax.random.key(seed), 5)
    own_keys = jax.random.split(jax.random.fold_in(keys[4], part), 5)
    return {
        "volume": noise(own_keys[0], (CHANNELS, DEPTH, HEIGHT, WIDTH), 1.0, 6.0, ((1, 16),)),
        "weight_two": noise(keys[1], (CHANNELS, CHANNELS, 3, 3, 3), (27 * CHANNELS) ** -0.5, 0.21875),
        "weight_three": noise(keys[2], (FILTERS, CHANNELS, 3, 3, 3), (27 * CHANNELS) ** -0.5, 0.21875),
        "cotangent": gaussian_with(own_keys[3], (FILTERS, DEPTH_HALF, HEIGHT_HALF, WIDTH_HALF), 1.0, 6.0, ((1, 16),), (1, 0, 16, 2.0)),
    }


layout_names = ('NCDHW', 'OIDHW', 'NCDHW')

def convolve(field, kernel):
    return lax.conv_general_dilated(field.astype(jnp.float32)[None], kernel.astype(jnp.float32), (1, 1, 1), [(1, 1), (1, 1), (1, 1)], dimension_numbers=layout_names, precision=lax.Precision.HIGHEST)[0]

def mirrored(kernel):
    return jnp.flip(jnp.transpose(kernel, (1, 0, 2, 3, 4)), (2, 3, 4))

def kernel_grad(field, upstream):
    padded = jnp.pad(field.astype(jnp.float32), ((0, 0), (1, 1), (1, 1), (1, 1)))
    result = lax.conv_general_dilated(padded[:, None], upstream.astype(jnp.float32)[:, None], (1, 1, 1), 'VALID', dimension_numbers=layout_names, precision=lax.Precision.HIGHEST)
    return jnp.transpose(result, (1, 0, 2, 3, 4))

def silu_slope(values):
    sigma = jax.nn.sigmoid(values)
    return sigma * (1.0 + values * (1.0 - sigma))

def reference(volume, weight_two, weight_three, cotangent):
    before = convolve(volume, weight_two)
    active = jax.nn.silu(before).astype(jnp.bfloat16)
    shape = active.shape
    pooled = active.astype(jnp.float32).reshape(shape[0], shape[1] // 2, 2, shape[2] // 2, 2, shape[3] // 2, 2).mean(axis=(2, 4, 6)).astype(jnp.bfloat16)
    features_three = convolve(pooled, weight_three).astype(jnp.bfloat16)
    grad_three = kernel_grad(pooled, cotangent)
    back_pooled = convolve(cotangent, mirrored(weight_three)).astype(jnp.bfloat16)
    spread = jnp.repeat(jnp.repeat(jnp.repeat(back_pooled.astype(jnp.float32), 2, 1), 2, 2), 2, 3) * 0.125
    back_before = (spread * silu_slope(before)).astype(jnp.bfloat16)
    grad_two = kernel_grad(volume, back_before)
    grad_volume = convolve(back_before, mirrored(weight_two)).astype(jnp.bfloat16)
    return (features_three, grad_three, grad_two, grad_volume)
```

```python
import functools

import jax
import jax.numpy as jnp
from jax import lax
from jax.experimental import pallas as pl
from jax.experimental.pallas import tpu as pltpu
from jax.sharding import PartitionSpec as P

BF = jnp.bfloat16
F32 = jnp.float32
LANES = 128
VMEM = pl.BlockSpec(memory_space=pltpu.VMEM)


def dot(a, b):
    return jnp.dot(a, b, preferred_element_type=F32)


def dot_nt(a, b):
    return lax.dot_general(a, b, (((1,), (1,)), ((), ())), preferred_element_type=F32)


def iota(shape, dim):
    return lax.broadcasted_iota(jnp.int32, shape, dim)


def place(rows, lanes, offset):
    return (iota((rows, lanes), 1) == iota((rows, lanes), 0) + offset).astype(F32).astype(BF)


def moved(x, step, width):
    lanes = x.shape[1]
    w = iota(x.shape, 1) % width
    rolled = pltpu.roll(x, (-step) % lanes, 1)
    edge = width - 1 if step > 0 else 0
    return jnp.where(w == edge, 0.0, rolled)


def taps_sum(y, rows, width):
    return y[rows : 2 * rows] + moved(y[:rows], -1, width) + moved(y[2 * rows :], 1, width)


def tap(d, h, w):
    return d * 9 + h * 3 + w


def unpack(src_ref, f_ref, halves):
    for half in range(halves):
        f_ref[half] = src_ref[:, half * LANES : (half + 1) * LANES].astype(F32)


def row_of(f_ref, start, count, stride, halves):
    parts = [f_ref[half, pl.ds(start, count, stride=stride), :] for half in range(halves)]
    whole = parts[0] if halves == 1 else jnp.concatenate(parts, axis=1)
    return whole.astype(BF)


def prep_kernel(C, F, H, W, w2, w3, x, cot, ka, kb, k3f, k3b, vown, cown, xf, cf):
    span = 4 * C
    ka[...] = jnp.zeros(ka.shape, BF)
    kb[...] = jnp.zeros(kb.shape, BF)
    k3f[...] = jnp.zeros(k3f.shape, BF)
    stacks = [w2[dt * 9 : dt * 9 + 9].reshape(9 * C, C) for dt in range(3)]
    eye_c = place(C, C, 0)
    zero_c = jnp.zeros((C, C), BF)
    for d in range(2):
        t_a = sum(dot(stacks[dt], place(C, span, (dt + d) * C)) for dt in range(3)).astype(BF)
        rows = []
        for wt in range(3):
            for ht in range(3):
                three = [w2[tap(2 - dt, 2 - ht, 2 - wt)] for dt in range(3)]
                rows += ([zero_c] + three) if d else (three + [zero_c])
        t_b = dot_nt(eye_c, jnp.concatenate(rows, axis=0)).astype(BF)
        for wt in range(3):
            for h in range(2):
                at = (wt * 4 + d * 2 + h) * C
                for ht in range(3):
                    lane = (h + ht) * span
                    g = ht * 3 + wt
                    ka[at : at + C, lane : lane + span] = t_a[g * C : g * C + C]
                    q = wt * 3 + ht
                    kb[at : at + C, lane : lane + span] = t_b[:, q * span : q * span + span]
    zero_f = jnp.zeros((C, F), BF)
    rows = []
    for wt in range(3):
        for ht in range(3):
            rows += [w3[tap(dt, ht, wt)] for dt in range(3)] + [zero_f]
    t_f = dot_nt(place(F, F, 0), jnp.concatenate(rows, axis=0)).astype(BF)
    for wt in range(3):
        for h in range(2):
            at = (wt * 2 + h) * F
            for ht in range(3):
                lane = (h + ht) * span
                q = wt * 3 + ht
                k3f[at : at + F, lane : lane + span] = t_f[:, q * span : q * span + span]
    wide = 4 * F
    picked = [
        jnp.concatenate([w3[tap(2 - dt, 2 - ht, 2 - wt)] for wt in range(3) for dt in range(3)], axis=0)
        for ht in range(3)
    ]
    for h in range(2):
        t_u = sum(dot(picked[ht], place(F, wide, (ht + h) * F)) for ht in range(3)).astype(BF)
        for wt in range(3):
            at = (wt * 2 + h) * C
            for dt in range(3):
                q = wt * 3 + dt
                k3b[at : at + C, dt * wide : dt * wide + wide] = t_u[q * C : q * C + C]
    halves = W // LANES
    unpack(x, xf, halves)
    for h in range(H):
        for d in range(2):
            vown[(h * 2 + d) * C : (h * 2 + d + 1) * C, :] = row_of(xf, d * H + h, C, 2 * H, halves)
    low = H // 2
    unpack(cot, cf, W // 2 // LANES)
    for h in range(low):
        cown[h * F : h * F + F, :] = row_of(cf, h, F, low, W // 2 // LANES)


def forward_kernel(C, F, H, W, xl, xr, cl, cr, vown, cown, ka, k3b, send_l, send_r, vv, cc, xf, cf, bp):
    halves, low, wide = W // LANES, H // 2, W // 2
    for plane, src in ((0, xl), (3, xr)):
        unpack(src, xf, halves)
        for h in range(H):
            tile = row_of(xf, h, C, H, halves)
            for b in range(low):
                j = h + 1 - 2 * b
                if 0 <= j < 4:
                    at = (j * 4 + plane) * C
                    vv[at : at + C, b * W : b * W + W] = tile
    for h in range(H):
        tile = vown[h * 2 * C : (h + 1) * 2 * C, :]
        for b in range(low):
            j = h + 1 - 2 * b
            if 0 <= j < 4:
                at = (j * 4 + 1) * C
                vv[at : at + 2 * C, b * W : b * W + W] = tile
    vv[: 4 * C, :W] = jnp.zeros((4 * C, W), BF)
    vv[12 * C :, (low - 1) * W :] = jnp.zeros((4 * C, W), BF)
    pairs = low // 2
    for plane, src in ((0, cl), (1, None), (2, cr)):
        if src is not None:
            unpack(src, cf, wide // LANES)
        for h in range(low):
            tile = cown[h * F : h * F + F, :] if src is None else row_of(cf, h, F, low, wide // LANES)
            for b in range(pairs):
                j = h + 1 - 2 * b
                if 0 <= j < 4:
                    at = (plane * 4 + j) * F
                    cc[at : at + F, b * wide : b * wide + wide] = tile
        cc[plane * 4 * F : plane * 4 * F + F, :wide] = jnp.zeros((F, wide), BF)
        cc[(plane * 4 + 3) * F : (plane * 4 + 4) * F, (pairs - 1) * wide :] = jnp.zeros((F, wide), BF)
    y = dot(k3b[...], cc[...])
    bp[...] = taps_sum(y, 2 * C, wide).astype(BF)
    eighth = jnp.where(iota((W, wide), 0) // 2 == iota((W, wide), 1), 0.125, 0.0).astype(BF)
    spread = jnp.where(iota((wide, W), 1) // 2 == iota((wide, W), 0), 0.125, 0.0).astype(BF)
    quarter = low // 2
    for b in range(low):
        y = dot(ka[...], vv[:, b * W : b * W + W])
        before = taps_sum(y, 4 * C, W)
        sigma = jax.nn.sigmoid(before)
        active = (before * sigma).astype(BF)
        sums = dot(active, eighth)
        pooled = (sums[:C] + sums[C : 2 * C] + sums[2 * C : 3 * C] + sums[3 * C :]).astype(BF)
        back = dot(bp[(b % 2) * C : (b % 2) * C + C, (b // 2) * wide : (b // 2) * wide + wide], spread)
        slope = sigma * (1.0 + before * (1.0 - sigma))
        grad = jnp.concatenate([back] * 4, axis=0) * slope
        grad = grad.astype(BF)
        send_l[b * 2 * C : (b + 1) * 2 * C, :] = grad[: 2 * C]
        send_r[b * 2 * C : (b + 1) * 2 * C, :] = grad[2 * C :]
        at, lane = H * C + (b % quarter) * C, (b // quarter) * wide
        send_l[at : at + C, lane : lane + wide] = pooled
        send_r[at : at + C, lane : lane + wide] = pooled


def grads_kernel(C, F, H, W, send_l, send_r, vv, cc, r2, r3, gg, ps):
    low, wide = H // 2, W // 2
    for b in range(low):
        for d, src in ((0, send_l), (1, send_r)):
            tile = src[b * 2 * C : (b + 1) * 2 * C, :]
            up = tile.astype(F32)
            for wt in range(3):
                val = tile if wt == 1 else moved(up, 1 - wt, W).astype(BF)
                at = (wt * 2 + d) * 2 * C
                gg[at : at + 2 * C, b * W : b * W + W] = val
    p2 = dot_nt(gg[...], vv[...])
    span = 4 * C
    for wt in range(3):
        for ht in range(3):
            parts = []
            for d in range(2):
                at = (wt * 4 + d * 2) * C
                parts.append(
                    p2[at : at + C, ht * span : ht * span + span]
                    + p2[at + C : at + 2 * C, (ht + 1) * span : (ht + 2) * span]
                )
            r2[wt * 3 + ht] = parts[0] + pltpu.roll(parts[1], span - C, 1)
    quarter = low // 2
    ps[...] = jnp.zeros(ps.shape, BF)
    for b in range(low // 2):
        for q in range(2):
            h = 2 * b + q
            at, lane = H * C + (h % quarter) * C, (h // quarter) * wide
            tile = send_l[at : at + C, lane : lane + wide]
            up = tile.astype(F32)
            for wt in range(3):
                val = tile if wt == 1 else moved(up, wt - 1, wide).astype(BF)
                to = (q * 4 + wt) * C
                ps[to : to + C, b * wide : b * wide + wide] = val
    p3 = dot_nt(cc[...], ps[...])
    for dt in range(3):
        for ht in range(3):
            first = ((2 - dt) * 4 + 2 - ht) * F
            second = first + F
            r3[dt * 3 + ht] = p3[first : first + F, :span] + p3[second : second + F, span:]


def backward_kernel(C, F, H, W, recv_l, recv_r, send_l, send_r, kb, k3f, gv, ft, gw, pp, zf, ff):
    low, wide = H // 2, W // 2
    quarter = low // 2
    sources = (recv_l, send_l, send_r, recv_r)
    gw[: 4 * C, :W] = jnp.zeros((4 * C, W), BF)
    gw[12 * C :, (low - 1) * W :] = jnp.zeros((4 * C, W), BF)
    for plane, src in enumerate(sources):
        for h in range(H):
            tile = src[h * C : h * C + C, :]
            for b in range(low):
                j = h + 1 - 2 * b
                if 0 <= j < 4:
                    at = (j * 4 + plane) * C
                    gw[at : at + C, b * W : b * W + W] = tile
    for b in range(low):
        y = dot(kb[...], gw[:, b * W : b * W + W])
        out = taps_sum(y, 4 * C, W)
        for d in range(2):
            for q in range(2):
                at = (d * 2 + q) * C
                for half in range(W // LANES):
                    zf[half, pl.ds(d * H + 2 * b + q, C, stride=2 * H), :] = out[
                        at : at + C, half * LANES : (half + 1) * LANES
                    ]
    for half in range(W // LANES):
        gv[:, half * LANES : (half + 1) * LANES] = zf[half].astype(BF)
    pp[...] = jnp.zeros(pp.shape, BF)
    for plane, src in ((0, recv_l), (1, send_l), (2, recv_r)):
        for h in range(low):
            at, lane = H * C + (h % quarter) * C, (h // quarter) * wide
            tile = src[at : at + C, lane : lane + wide]
            for b in range(low // 2):
                j = h + 1 - 2 * b
                if 0 <= j < 4:
                    to = (j * 4 + plane) * C
                    pp[to : to + C, b * wide : b * wide + wide] = tile
    y = dot(k3f[...], pp[...])
    out = taps_sum(y, 2 * F, wide)
    for b in range(low // 2):
        for q in range(2):
            for half in range(wide // LANES):
                lane = b * wide + half * LANES
                ff[half, pl.ds(2 * b + q, F, stride=low), :] = out[q * F : q * F + F, lane : lane + LANES]
    for half in range(wide // LANES):
        ft[:, half * LANES : (half + 1) * LANES] = ff[half].astype(BF)


def call(body, outs, scratch, flops, name, *args):
    moved_bytes = sum(a.size * a.dtype.itemsize for a in args)
    return pl.pallas_call(
        body,
        out_shape=outs,
        in_specs=[VMEM] * len(args),
        out_specs=jax.tree.map(lambda _: VMEM, outs),
        scratch_shapes=scratch,
        cost_estimate=pl.CostEstimate(flops=flops, bytes_accessed=moved_bytes, transcendentals=0),
        name=name,
    )(*args)


def exchange(to_left, to_right, axis):
    count = lax.axis_size(axis)
    from_left = lax.ppermute(to_right, axis, [(i, i + 1) for i in range(count - 1)])
    from_right = lax.ppermute(to_left, axis, [(i + 1, i) for i in range(count - 1)])
    return from_left, from_right


def reduce_both(full, parts, axis):
    count = lax.axis_size(axis)
    if count & (count - 1):
        return lax.psum(full, axis), lax.psum_scatter(parts, axis, scatter_dimension=1, tiled=True)
    g, o, lanes = parts.shape
    each = o // count
    index = lax.axis_index(axis)
    left = parts.reshape(g, count, each, lanes)
    step = 1
    while step < count:
        bit = (index // step) % 2
        split = left.reshape(g, left.shape[1] // 2, 2, each, lanes)
        keep = lax.dynamic_index_in_dim(split, bit, 2, keepdims=False)
        give = lax.dynamic_index_in_dim(split, 1 - bit, 2, keepdims=False)
        mine = full.astype(BF)
        packet = jnp.concatenate([mine.reshape(-1, lanes), give.astype(BF).reshape(-1, lanes)], axis=0)
        got = lax.ppermute(packet, axis, [(i, i ^ step) for i in range(count)])
        rows = full.shape[0] * full.shape[1]
        full = mine.astype(F32) + got[:rows].reshape(full.shape).astype(F32)
        left = keep + got[rows:].reshape(keep.shape).astype(F32)
        step *= 2
    return full, left[:, 0]


def local(volume, weight_two, weight_three, cotangent):
    C, planes, H, W = volume.shape
    F, _, low, wide = cotangent.shape
    assert planes == 2 and 2 * low == H and 2 * wide == W
    sds = jax.ShapeDtypeStruct
    w2 = jnp.transpose(weight_two, (2, 3, 4, 0, 1)).reshape(27, C, C)
    w3 = jnp.transpose(weight_three, (2, 3, 4, 1, 0)).reshape(27, C, F)
    x = volume.reshape(C * 2 * H, W)
    cot = cotangent.reshape(F * low, wide)
    first = volume[:, 0].reshape(C * H, W)
    last = volume[:, 1].reshape(C * H, W)
    xl, xr = exchange(first, last, "gx")
    cl, cr = exchange(cot, cot, "gx")
    halves, low_halves = W // LANES, wide // LANES
    bind = lambda body: functools.partial(body, C, F, H, W)
    ka, kb, k3f, k3b, vown, cown = call(
        bind(prep_kernel),
        (
            sds((12 * C, 16 * C), BF),
            sds((12 * C, 16 * C), BF),
            sds((6 * F, 16 * C), BF),
            sds((6 * C, 12 * F), BF),
            sds((H * 2 * C, W), BF),
            sds((low * F, wide), BF),
        ),
        [pltpu.VMEM((halves, C * 2 * H, LANES), F32), pltpu.VMEM((low_halves, F * low, LANES), F32)],
        400_000_000,
        "prep",
        w2,
        w3,
        x,
        cot,
    )
    send_l, send_r, vv, cc = call(
        bind(forward_kernel),
        (
            sds((H * C + low // 2 * C, W), BF),
            sds((H * C + low // 2 * C, W), BF),
            sds((16 * C, low * W), BF),
            sds((12 * F, low // 2 * wide), BF),
        ),
        [
            pltpu.VMEM((halves, C * H, LANES), F32),
            pltpu.VMEM((low_halves, F * low, LANES), F32),
            pltpu.VMEM((2 * C, low // 2 * wide), BF),
        ],
        1_500_000_000,
        "forward",
        xl,
        xr,
        cl,
        cr,
        vown,
        cown,
        ka,
        k3b,
    )
    recv_l, recv_r = exchange(send_l, send_r, "gx")
    r2, r3 = call(
        bind(grads_kernel),
        (sds((9, C, 4 * C), F32), sds((9, F, 4 * C), F32)),
        [pltpu.VMEM((12 * C, low * W), BF), pltpu.VMEM((8 * C, low // 2 * wide), BF)],
        1_200_000_000,
        "grads",
        send_l,
        send_r,
        vv,
        cc,
    )
    g2, g3 = reduce_both(r2, r3, "gx")
    gv, ft = call(
        bind(backward_kernel),
        (sds((C * 2 * H, W), BF), sds((F * low, wide), BF)),
        [
            pltpu.VMEM((16 * C, low * W), BF),
            pltpu.VMEM((16 * C, low // 2 * wide), BF),
            pltpu.VMEM((halves, C * 2 * H, LANES), F32),
            pltpu.VMEM((low_halves, F * low, LANES), F32),
        ],
        1_200_000_000,
        "backward",
        recv_l,
        recv_r,
        send_l,
        send_r,
        kb,
        k3f,
    )
    g2 = g2.reshape(3, 3, C, 4, C)[:, :, :, :3]
    grad_two = jnp.transpose(g2, (2, 4, 3, 1, 0))
    g3 = g3.reshape(3, 3, g3.shape[1], 4, C)[:, :, :, :3]
    grad_three = jnp.transpose(g3, (2, 4, 0, 1, 3))
    return (
        ft.reshape(F, 1, low, wide),
        grad_three,
        grad_two,
        gv.reshape(C, 2, H, W),
    )


def solution(mesh):
    return jax.shard_map(
        local,
        mesh=mesh,
        in_specs=(
            P(None, ("groups", "gx"), None, None),
            P(),
            P(),
            P(None, ("groups", "gx"), None, None),
        ),
        out_specs=(
            P(None, ("groups", "gx"), None, None),
            P(("groups", "gx"), None, None, None, None),
            P("groups", None, None, None, None),
            P(None, ("groups", "gx"), None, None),
        ),
        check_vma=False,
    )
```

```python
import functools

import jax
import jax.numpy as jnp
from jax import lax
from jax.experimental import pallas as pl
from jax.experimental.pallas import tpu as pltpu
from jax.sharding import PartitionSpec as P

BF = jnp.bfloat16
F32 = jnp.float32
LANES = 128
VMEM = pl.BlockSpec(memory_space=pltpu.VMEM)


def dot(a, b):
    return jnp.dot(a, b, preferred_element_type=F32)


def dot_nt(a, b):
    return lax.dot_general(a, b, (((1,), (1,)), ((), ())), preferred_element_type=F32)


def iota(shape, dim):
    return lax.broadcasted_iota(jnp.int32, shape, dim)


def place(rows, lanes, offset):
    return (iota((rows, lanes), 1) == iota((rows, lanes), 0) + offset).astype(F32).astype(BF)


def moved(x, step, width):
    lanes = x.shape[1]
    w = iota(x.shape, 1) % width
    rolled = pltpu.roll(x, (-step) % lanes, 1)
    edge = width - 1 if step > 0 else 0
    return jnp.where(w == edge, 0.0, rolled)


def taps_sum(y, rows, width):
    return y[rows : 2 * rows] + moved(y[:rows], -1, width) + moved(y[2 * rows :], 1, width)


def tap(d, h, w):
    return d * 9 + h * 3 + w


def unpack(src_ref, f_ref, halves):
    for half in range(halves):
        f_ref[half] = src_ref[:, half * LANES : (half + 1) * LANES].astype(F32)


def row_of(f_ref, start, count, stride, first, last):
    parts = [f_ref[half, pl.ds(start, count, stride=stride), :] for half in range(first, last)]
    whole = parts[0] if len(parts) == 1 else jnp.concatenate(parts, axis=1)
    return whole.astype(BF)


def prep_kernel(C, F, H, W, w2, w3, x, cot, ka, kb, k3f, k3b, vown, cown, xf, cf):
    span = 4 * C
    ka[...] = jnp.zeros(ka.shape, BF)
    kb[...] = jnp.zeros(kb.shape, BF)
    k3f[...] = jnp.zeros(k3f.shape, BF)
    stacks = [w2[dt * 9 : dt * 9 + 9].reshape(9 * C, C) for dt in range(3)]
    eye_c = place(C, C, 0)
    zero_c = jnp.zeros((C, C), BF)
    for d in range(2):
        t_a = sum(dot(stacks[dt], place(C, span, (dt + d) * C)) for dt in range(3)).astype(BF)
        rows = []
        for wt in range(3):
            for ht in range(3):
                three = [w2[tap(2 - dt, 2 - ht, 2 - wt)] for dt in range(3)]
                rows += ([zero_c] + three) if d else (three + [zero_c])
        t_b = dot_nt(eye_c, jnp.concatenate(rows, axis=0)).astype(BF)
        for wt in range(3):
            for h in range(2):
                at = (wt * 4 + d * 2 + h) * C
                for ht in range(3):
                    lane = (h + ht) * span
                    g = ht * 3 + wt
                    ka[at : at + C, lane : lane + span] = t_a[g * C : g * C + C]
                    q = wt * 3 + ht
                    kb[at : at + C, lane : lane + span] = t_b[:, q * span : q * span + span]
    zero_f = jnp.zeros((C, F), BF)
    rows = []
    for wt in range(3):
        for ht in range(3):
            rows += [w3[tap(dt, ht, wt)] for dt in range(3)] + [zero_f]
    t_f = dot_nt(place(F, F, 0), jnp.concatenate(rows, axis=0)).astype(BF)
    for wt in range(3):
        for h in range(2):
            at = (wt * 2 + h) * F
            for ht in range(3):
                lane = (h + ht) * span
                q = wt * 3 + ht
                k3f[at : at + F, lane : lane + span] = t_f[:, q * span : q * span + span]
    wide = 4 * F
    picked = [
        jnp.concatenate([w3[tap(2 - dt, 2 - ht, 2 - wt)] for wt in range(3) for dt in range(3)], axis=0)
        for ht in range(3)
    ]
    for h in range(2):
        t_u = sum(dot(picked[ht], place(F, wide, (ht + h) * F)) for ht in range(3)).astype(BF)
        for wt in range(3):
            at = (wt * 2 + h) * C
            for dt in range(3):
                q = wt * 3 + dt
                k3b[at : at + C, dt * wide : dt * wide + wide] = t_u[q * C : q * C + C]
    halves = W // LANES
    unpack(x, xf, halves)
    for h in range(H):
        for d in range(2):
            vown[(h * 2 + d) * C : (h * 2 + d + 1) * C, :] = row_of(xf, d * H + h, C, 2 * H, 0, halves)
    low = H // 2
    unpack(cot, cf, W // 2 // LANES)
    for h in range(low):
        cown[h * F : h * F + F, :] = row_of(cf, h, F, low, 0, W // 2 // LANES)


def parity():
    return lax.axis_index("gx") % 2


def forward_kernel(C, F, H, W, a1, a2, vown, cown, ka, k3b, g, p1, p2, vv, cc, xf, bp):
    halves, low, wide = W // LANES, H // 2, W // 2
    total = halves + wide // LANES
    odd = parity()
    pairs = low // 2
    for src, flip in ((a1, odd), (a2, 1 - odd)):
        unpack(src, xf, total)
        plane = 3 - 3 * flip
        for h in range(H):
            tile = row_of(xf, h, C, H, 0, halves)
            for b in range(low):
                j = h + 1 - 2 * b
                if 0 <= j < 4:
                    at = pl.multiple_of((j * 4 + plane) * C, C)
                    vv[pl.ds(at, C), b * W : b * W + W] = tile
        plane = 2 - 2 * flip
        for h in range(low):
            tile = row_of(xf, h, F, low, halves, total)
            for b in range(pairs):
                j = h + 1 - 2 * b
                if 0 <= j < 4:
                    at = pl.multiple_of((plane * 4 + j) * F, F)
                    cc[pl.ds(at, F), b * wide : b * wide + wide] = tile
    for h in range(H):
        tile = vown[h * 2 * C : (h + 1) * 2 * C, :]
        for b in range(low):
            j = h + 1 - 2 * b
            if 0 <= j < 4:
                at = (j * 4 + 1) * C
                vv[at : at + 2 * C, b * W : b * W + W] = tile
    vv[: 4 * C, :W] = jnp.zeros((4 * C, W), BF)
    vv[12 * C :, (low - 1) * W :] = jnp.zeros((4 * C, W), BF)
    for h in range(low):
        tile = cown[h * F : h * F + F, :]
        for b in range(pairs):
            j = h + 1 - 2 * b
            if 0 <= j < 4:
                cc[(4 + j) * F : (5 + j) * F, b * wide : b * wide + wide] = tile
    for plane in range(3):
        cc[plane * 4 * F : plane * 4 * F + F, :wide] = jnp.zeros((F, wide), BF)
        cc[(plane * 4 + 3) * F : (plane * 4 + 4) * F, (pairs - 1) * wide :] = jnp.zeros((F, wide), BF)
    y = dot(k3b[...], cc[...])
    bp[...] = taps_sum(y, 2 * C, wide).astype(BF)
    eighth = jnp.where(iota((W, wide), 0) // 2 == iota((W, wide), 1), 0.125, 0.0).astype(BF)
    spread = jnp.where(iota((wide, W), 1) // 2 == iota((wide, W), 0), 0.125, 0.0).astype(BF)
    quarter = low // 2
    for b in range(low):
        y = dot(ka[...], vv[:, b * W : b * W + W])
        before = taps_sum(y, 4 * C, W)
        sigma = jax.nn.sigmoid(before)
        active = (before * sigma).astype(BF)
        sums = dot(active, eighth)
        pooled = (sums[:C] + sums[C : 2 * C] + sums[2 * C : 3 * C] + sums[3 * C :]).astype(BF)
        back = dot(bp[(b % 2) * C : (b % 2) * C + C, (b // 2) * wide : (b // 2) * wide + wide], spread)
        slope = sigma * (1.0 + before * (1.0 - sigma))
        grad = jnp.concatenate([back] * 4, axis=0) * slope
        grad = grad.astype(BF)
        at, lane = H * C + (b % quarter) * C, (b // quarter) * wide
        for d in range(2):
            g[d, b * 2 * C : (b + 1) * 2 * C, :] = grad[d * 2 * C : (d + 1) * 2 * C]
            g[d, at : at + C, lane : lane + wide] = pooled
    p1[...] = g[1 - odd]
    p2[...] = g[odd]


def grads_kernel(C, F, H, W, count, g, vv, cc, packet, keep, gg, ps, r3):
    low, wide = H // 2, W // 2
    for b in range(low):
        for d in range(2):
            tile = g[d, b * 2 * C : (b + 1) * 2 * C, :]
            up = tile.astype(F32)
            for wt in range(3):
                val = tile if wt == 1 else moved(up, 1 - wt, W).astype(BF)
                at = (wt * 2 + d) * 2 * C
                gg[at : at + 2 * C, b * W : b * W + W] = val
    p2 = dot_nt(gg[...], vv[...])
    span = 4 * C
    for wt in range(3):
        for ht in range(3):
            parts = []
            for d in range(2):
                at = (wt * 4 + d * 2) * C
                parts.append(
                    p2[at : at + C, ht * span : ht * span + span]
                    + p2[at + C : at + 2 * C, (ht + 1) * span : (ht + 2) * span]
                )
            to = (wt * 3 + ht) * C
            packet[to : to + C, :] = (parts[0] + pltpu.roll(parts[1], span - C, 1)).astype(BF)
    quarter = low // 2
    ps[...] = jnp.zeros(ps.shape, BF)
    for b in range(low // 2):
        for q in range(2):
            h = 2 * b + q
            at, lane = H * C + (h % quarter) * C, (h // quarter) * wide
            tile = g[0, at : at + C, lane : lane + wide]
            up = tile.astype(F32)
            for wt in range(3):
                val = tile if wt == 1 else moved(up, wt - 1, wide).astype(BF)
                to = (q * 4 + wt) * C
                ps[to : to + C, b * wide : b * wide + wide] = val
    p3 = dot_nt(cc[...], ps[...])
    tiles = []
    for dt in range(3):
        for ht in range(3):
            first = ((2 - dt) * 4 + 2 - ht) * F
            second = first + F
            tiles.append(p3[first : first + F, :span] + p3[second : second + F, span:])
    each = F // count
    row, col = iota((F, F), 0), iota((F, F), 1)
    chunk, index, step = row // each, jnp.zeros((F, F), jnp.int32), 1
    while step < count:
        index = index * 2 + chunk % 2
        chunk, step = chunk // 2, step * 2
    order = (col == index * each + row % each).astype(F32).astype(BF)
    r3[...] = dot(order, jnp.concatenate(tiles, axis=1).astype(BF))
    half = F // 2
    odd = parity()
    for q in range(9):
        to = 9 * C + q * half
        lanes = slice(q * span, q * span + span)
        packet[to : to + half, :] = r3[pl.ds(pl.multiple_of((1 - odd) * half, half), half), lanes].astype(BF)
        keep[q] = r3[pl.ds(pl.multiple_of(odd * half, half), half), lanes]


def backward_kernel(C, F, H, W, b1, b2, g, kb, k3f, gv, ft, gw, pp, zf, ff):
    low, wide = H // 2, W // 2
    quarter = low // 2
    odd = parity()
    near, far = 3 - 3 * odd, 3 * odd
    sources = ((near, b1), (far, b2), (1, g.at[0]), (2, g.at[1]))
    gw[: 4 * C, :W] = jnp.zeros((4 * C, W), BF)
    gw[12 * C :, (low - 1) * W :] = jnp.zeros((4 * C, W), BF)
    for plane, src in sources:
        for h in range(H):
            tile = src[h * C : h * C + C, :]
            for b in range(low):
                j = h + 1 - 2 * b
                if 0 <= j < 4:
                    at = pl.multiple_of((j * 4 + plane) * C, C)
                    gw[pl.ds(at, C), b * W : b * W + W] = tile
    for b in range(low):
        y = dot(kb[...], gw[:, b * W : b * W + W])
        out = taps_sum(y, 4 * C, W)
        for d in range(2):
            for q in range(2):
                at = (d * 2 + q) * C
                for half in range(W // LANES):
                    zf[half, pl.ds(d * H + 2 * b + q, C, stride=2 * H), :] = out[
                        at : at + C, half * LANES : (half + 1) * LANES
                    ]
    for half in range(W // LANES):
        gv[:, half * LANES : (half + 1) * LANES] = zf[half].astype(BF)
    pp[...] = jnp.zeros(pp.shape, BF)
    near, far = 2 - 2 * odd, 2 * odd
    for plane, src in ((near, b1), (far, b2), (1, g.at[0])):
        for h in range(low):
            at, lane = H * C + (h % quarter) * C, (h // quarter) * wide
            tile = src[at : at + C, lane : lane + wide]
            for b in range(low // 2):
                j = h + 1 - 2 * b
                if 0 <= j < 4:
                    to = pl.multiple_of((j * 4 + plane) * C, C)
                    pp[pl.ds(to, C), b * wide : b * wide + wide] = tile
    y = dot(k3f[...], pp[...])
    out = taps_sum(y, 2 * F, wide)
    for b in range(low // 2):
        for q in range(2):
            for half in range(wide // LANES):
                lane = b * wide + half * LANES
                ff[half, pl.ds(2 * b + q, F, stride=low), :] = out[q * F : q * F + F, lane : lane + LANES]
    for half in range(wide // LANES):
        ft[:, half * LANES : (half + 1) * LANES] = ff[half].astype(BF)


def call(body, outs, scratch, flops, name, *args):
    moved_bytes = sum(a.size * a.dtype.itemsize for a in args)
    return pl.pallas_call(
        body,
        out_shape=outs,
        in_specs=[VMEM] * len(args),
        out_specs=jax.tree.map(lambda _: VMEM, outs),
        scratch_shapes=scratch,
        cost_estimate=pl.CostEstimate(flops=flops, bytes_accessed=moved_bytes, transcendentals=0),
        compiler_params=pltpu.CompilerParams(vmem_limit_bytes=24 * 2**20),
        name=name,
    )(*args)


def swap(near, far, axis):
    count = lax.axis_size(axis)
    pairs = [(i, i + 1) for i in range(1, count - 1, 2)]
    got_far = lax.ppermute(far, axis, pairs + [(b, a) for a, b in pairs])
    pairs = [(i, i + 1) for i in range(0, count - 1, 2)]
    got_near = lax.ppermute(near, axis, pairs + [(b, a) for a, b in pairs])
    return got_near, got_far


def reduce_both(packet, keep, rows, axis):
    count = lax.axis_size(axis)
    index = lax.axis_index(axis)
    step = 1
    full = packet[:rows]
    while step < count:
        got = lax.ppermute(packet, axis, [(i, i ^ step) for i in range(count)])
        full = full.astype(F32) + got[:rows].astype(F32)
        keep = keep + got[rows:].reshape(keep.shape).astype(F32)
        step *= 2
        if step < count:
            full = full.astype(BF)
            half = keep.shape[1] // 2
            bit = (index // step) % 2
            give = lax.dynamic_slice_in_dim(keep, (1 - bit) * half, half, 1)
            keep = lax.dynamic_slice_in_dim(keep, bit * half, half, 1)
            packet = jnp.concatenate([full, give.astype(BF).reshape(-1, full.shape[1])], axis=0)
    return full, keep


def local(volume, weight_two, weight_three, cotangent):
    C, planes, H, W = volume.shape
    F, _, low, wide = cotangent.shape
    count = lax.axis_size("gx")
    assert planes == 2 and 2 * low == H and 2 * wide == W
    assert count & (count - 1) == 0 and F % count == 0 and C * H == F * low
    sds = jax.ShapeDtypeStruct
    odd = lax.axis_index("gx") % 2
    w2 = jnp.transpose(weight_two, (2, 3, 4, 0, 1)).reshape(27, C, C)
    w3 = jnp.transpose(weight_three, (2, 3, 4, 1, 0)).reshape(27, C, F)
    x = volume.reshape(C * 2 * H, W)
    cot = cotangent.reshape(F * low, wide)
    near = lax.dynamic_index_in_dim(volume, 1 - odd, 1, keepdims=False).reshape(C * H, W)
    far = lax.dynamic_index_in_dim(volume, odd, 1, keepdims=False).reshape(C * H, W)
    with jax.named_scope("halo_a"):
        a1, a2 = swap(jnp.concatenate([near, cot], axis=1), jnp.concatenate([far, cot], axis=1), "gx")
    halves, low_halves = W // LANES, wide // LANES
    bind = lambda body, *more: functools.partial(body, C, F, H, W, *more)
    ka, kb, k3f, k3b, vown, cown = call(
        bind(prep_kernel),
        (
            sds((12 * C, 16 * C), BF),
            sds((12 * C, 16 * C), BF),
            sds((6 * F, 16 * C), BF),
            sds((6 * C, 12 * F), BF),
            sds((H * 2 * C, W), BF),
            sds((low * F, wide), BF),
        ),
        [pltpu.VMEM((halves, C * 2 * H, LANES), F32), pltpu.VMEM((low_halves, F * low, LANES), F32)],
        400_000_000,
        "prep",
        w2,
        w3,
        x,
        cot,
    )
    rows = H * C + low // 2 * C
    g, p1, p2, vv, cc = call(
        bind(forward_kernel),
        (
            sds((2, rows, W), BF),
            sds((rows, W), BF),
            sds((rows, W), BF),
            sds((16 * C, low * W), BF),
            sds((12 * F, low // 2 * wide), BF),
        ),
        [
            pltpu.VMEM((halves + low_halves, C * H, LANES), F32),
            pltpu.VMEM((2 * C, low // 2 * wide), BF),
        ],
        1_500_000_000,
        "forward",
        a1,
        a2,
        vown,
        cown,
        ka,
        k3b,
    )
    with jax.named_scope("halo_b"):
        b1, b2 = swap(p1, p2, "gx")
    packet, keep = call(
        bind(grads_kernel, count),
        (sds((9 * C + 9 * F // 2, 4 * C), BF), sds((9, F // 2, 4 * C), F32)),
        [
            pltpu.VMEM((12 * C, low * W), BF),
            pltpu.VMEM((8 * C, low // 2 * wide), BF),
            pltpu.VMEM((F, 36 * C), F32),
        ],
        1_200_000_000,
        "grads",
        g,
        vv,
        cc,
    )
    g2, g3 = reduce_both(packet, keep, 9 * C, "gx")
    gv, ft = call(
        bind(backward_kernel),
        (sds((C * 2 * H, W), BF), sds((F * low, wide), BF)),
        [
            pltpu.VMEM((16 * C, low * W), BF),
            pltpu.VMEM((16 * C, low // 2 * wide), BF),
            pltpu.VMEM((halves, C * 2 * H, LANES), F32),
            pltpu.VMEM((low_halves, F * low, LANES), F32),
        ],
        1_200_000_000,
        "backward",
        b1,
        b2,
        g,
        kb,
        k3f,
    )
    g2 = g2.reshape(3, 3, C, 4, C)[:, :, :, :3]
    grad_two = jnp.transpose(g2, (2, 4, 3, 1, 0))
    g3 = g3.reshape(3, 3, g3.shape[1], 4, C)[:, :, :, :3]
    grad_three = jnp.transpose(g3, (2, 4, 0, 1, 3))
    return (
        ft.reshape(F, 1, low, wide),
        grad_three,
        grad_two,
        gv.reshape(C, 2, H, W),
    )


def solution(mesh):
    return jax.shard_map(
        local,
        mesh=mesh,
        in_specs=(
            P(None, ("groups", "gx"), None, None),
            P(),
            P(),
            P(None, ("groups", "gx"), None, None),
        ),
        out_specs=(
            P(None, ("groups", "gx"), None, None),
            P(("groups", "gx"), None, None, None, None),
            P("groups", None, None, None, None),
            P(None, ("groups", "gx"), None, None),
        ),
        check_vma=False,
    )
```

```python
import functools

import jax
import jax.numpy as jnp
from jax import lax
from jax.experimental import pallas as pl
from jax.experimental.pallas import tpu as pltpu
from jax.sharding import PartitionSpec as P


BF = jnp.bfloat16
F32 = jnp.float32
LANES = 128
VMEM = pl.BlockSpec(memory_space=pltpu.VMEM)


def dot(a, b):
    return jnp.dot(a, b, preferred_element_type=F32)


def dot_nt(a, b):
    return lax.dot_general(a, b, (((1,), (1,)), ((), ())), preferred_element_type=F32)


def iota(shape, dim):
    return lax.broadcasted_iota(jnp.int32, shape, dim)


def place(rows, lanes, offset):
    return (iota((rows, lanes), 1) == iota((rows, lanes), 0) + offset).astype(F32).astype(BF)


def moved(x, step, width):
    lanes = x.shape[1]
    w = iota(x.shape, 1) % width
    rolled = pltpu.roll(x, (-step) % lanes, 1)
    edge = width - 1 if step > 0 else 0
    return jnp.where(w == edge, 0.0, rolled)


def taps_sum(y, rows, width):
    return y[rows : 2 * rows] + moved(y[:rows], -1, width) + moved(y[2 * rows :], 1, width)


def tap(d, h, w):
    return d * 9 + h * 3 + w


def unpack(src_ref, f_ref, halves, scale=None):
    for half in range(halves):
        part = src_ref[:, half * LANES : (half + 1) * LANES].astype(F32)
        f_ref[half] = part if scale is None else part * scale


def row_of(f_ref, start, count, stride, first, last):
    parts = [f_ref[half, pl.ds(start, count, stride=stride), :] for half in range(first, last)]
    whole = parts[0] if len(parts) == 1 else jnp.concatenate(parts, axis=1)
    return whole.astype(BF)


def windows(h, pairs):
    return [(b, h + 1 - 2 * b) for b in range(pairs) if 0 <= h + 1 - 2 * b < 4]


def parity():
    return lax.axis_index("gx") % 2


def inside():
    index = lax.axis_index("gx")
    return jnp.where((index == 0) | (index == lax.axis_size("gx") - 1), 0.0, 1.0)


def fill_plane(dst, tile_of, rows, pairs, planes, plane, height, width):
    for h in range(rows):
        tile = tile_of(h)
        for b, j in windows(h, pairs):
            at = pl.multiple_of((j * planes + plane) * height, height)
            dst[pl.ds(at, height), b * width : b * width + width] = tile


def clear_ends(dst, planes, height, pairs, width):
    dst[: planes * height, :width] = jnp.zeros((planes * height, width), BF)
    dst[3 * planes * height :, (pairs - 1) * width :] = jnp.zeros((planes * height, width), BF)


def near_kernel(C, F, H, W, w2, near, far, a1, ka, vv, slope, means, xf):
    span = 4 * C
    halves, low = W // LANES, H // 2
    odd = parity()
    ka[...] = jnp.zeros(ka.shape, BF)
    stacks = [w2[dt * 9 : dt * 9 + 9].reshape(9 * C, C) for dt in range(3)]
    for d in range(2):
        tiles = sum(dot(stacks[dt], place(C, span, (dt + d) * C)) for dt in range(3)).astype(BF)
        for wt in range(3):
            for h in range(2):
                at = (wt * 2 + h) * C
                for ht in range(3):
                    lane = (h + ht) * span
                    g = ht * 3 + wt
                    ka[d, at : at + C, lane : lane + span] = tiles[g * C : g * C + C]
    for src, plane in ((near, 2 - odd), (far, 1 + odd), (a1, 3 - 3 * odd)):
        unpack(src, xf, halves)
        fill_plane(vv, lambda h: row_of(xf, h, C, H, 0, halves), H, low, 4, plane, C, W)
    zero = jnp.zeros((C, W), BF)
    fill_plane(vv, lambda h: zero, H, low, 4, 3 * odd, C, W)
    clear_ends(vv, 4, C, low, W)
    forward_plane(C, H, W, ka, 1 - odd, vv, slope, lambda b, mean: means.__setitem__(b, mean))


def forward_plane(C, H, W, ka, d, vv, slope, put):
    wide = W // 2
    eighth = jnp.where(iota((W, wide), 0) // 2 == iota((W, wide), 1), 0.125, 0.0).astype(BF)
    for b in range(H // 2):
        value = taps_sum(dot(ka[d], vv[:, b * W : b * W + W]), 2 * C, W)
        sigma = jax.nn.sigmoid(value)
        slope[b] = sigma * (1.0 + value * (1.0 - sigma))
        sums = dot((value * sigma).astype(BF), eighth)
        put(b, sums[:C] + sums[C:])


def far_kernel(C, F, H, W, a2, ka, means, vv_in, slope, pooled, vv, xf):
    halves, low, wide = W // LANES, H // 2, W // 2
    odd = parity()
    unpack(a2, xf, halves, inside())
    fill_plane(vv, lambda h: row_of(xf, h, C, H, 0, halves), H, low, 4, 3 * odd, C, W)
    quarter = low // 2

    def put(b, mean):
        at, lane = (b % quarter) * C, (b // quarter) * wide
        pooled[at : at + C, lane : lane + wide] = (mean + means[b]).astype(BF)

    forward_plane(C, H, W, ka, odd, vv, slope, put)


def prep_kernel(C, F, H, W, w2, w3, cot, kb, k3f, k3b, cc, cf):
    span, low, wide = 4 * C, H // 2, W // 2
    kb[...] = jnp.zeros(kb.shape, BF)
    k3f[...] = jnp.zeros(k3f.shape, BF)
    eye_c = place(C, C, 0)
    zero_c = jnp.zeros((C, C), BF)
    for d in range(2):
        rows = []
        for wt in range(3):
            for ht in range(3):
                three = [w2[tap(2 - dt, 2 - ht, 2 - wt)] for dt in range(3)]
                rows += ([zero_c] + three) if d else (three + [zero_c])
        tiles = dot_nt(eye_c, jnp.concatenate(rows, axis=0)).astype(BF)
        for wt in range(3):
            for h in range(2):
                at = (wt * 2 + h) * C
                for ht in range(3):
                    lane = (h + ht) * span
                    q = wt * 3 + ht
                    kb[d, at : at + C, lane : lane + span] = tiles[:, q * span : q * span + span]
    zero_f = jnp.zeros((C, F), BF)
    rows = []
    for wt in range(3):
        for ht in range(3):
            rows += [w3[tap(dt, ht, wt)] for dt in range(3)] + [zero_f]
    tiles = dot_nt(place(F, F, 0), jnp.concatenate(rows, axis=0)).astype(BF)
    for wt in range(3):
        for h in range(2):
            at = (wt * 2 + h) * F
            for ht in range(3):
                lane = (h + ht) * span
                q = wt * 3 + ht
                k3f[at : at + F, lane : lane + span] = tiles[:, q * span : q * span + span]
    four = 4 * F
    picked = [
        jnp.concatenate([w3[tap(2 - dt, 2 - ht, 2 - wt)] for wt in range(3) for dt in range(3)], axis=0)
        for ht in range(3)
    ]
    for h in range(2):
        tiles = sum(dot(picked[ht], place(F, four, (ht + h) * F)) for ht in range(3)).astype(BF)
        for wt in range(3):
            at = (wt * 2 + h) * C
            for dt in range(3):
                q = wt * 3 + dt
                k3b[at : at + C, dt * four : dt * four + four] = tiles[q * C : q * C + C]
    unpack(cot, cf, wide // LANES)
    fill_cot(F, H, W, cc, cf, 1)
    for plane in range(3):
        cc[plane * four : plane * four + F, :wide] = jnp.zeros((F, wide), BF)
        cc[plane * four + 3 * F : plane * four + four, (low // 2 - 1) * wide :] = jnp.zeros((F, wide), BF)


def fill_cot(F, H, W, cc, cf, plane):
    low, wide = H // 2, W // 2
    for h in range(low):
        tile = row_of(cf, h, F, low, 0, wide // LANES)
        for b, j in windows(h, low // 2):
            at = pl.multiple_of((plane * 4 + j) * F, F)
            cc[pl.ds(at, F), b * wide : b * wide + wide] = tile


def slope_kernel(C, F, H, W, c1, c2, slope_near, slope_far, pooled, k3b, cc_in, p1, p2, cc, cf, bp):
    low, wide = H // 2, W // 2
    odd = parity()
    for src, plane, scale in ((c1, 2 - 2 * odd, None), (c2, 2 * odd, inside())):
        unpack(src, cf, wide // LANES, scale)
        fill_cot(F, H, W, cc, cf, plane)
    bp[...] = taps_sum(dot(k3b[...], cc[...]), 2 * C, wide).astype(BF)
    spread = jnp.where(iota((wide, W), 1) // 2 == iota((wide, W), 0), 0.125, 0.0).astype(BF)
    for b in range(low):
        back = dot(bp[(b % 2) * C : (b % 2) * C + C, (b // 2) * wide : (b // 2) * wide + wide], spread)
        back = jnp.concatenate([back, back], axis=0)
        for out, slope in ((p1, slope_near), (p2, slope_far)):
            out[b * 2 * C : (b + 1) * 2 * C, :] = (back * slope[b]).astype(BF)
    for out in (p1, p2):
        out[H * C :, :] = pooled[...]


def grads_kernel(C, F, H, W, count, p1, p2, vv, cc, packet, keep, gg, ps, r2, r3):
    low, wide = H // 2, W // 2
    odd = parity()
    for b in range(low):
        for d, src in ((1 - odd, p1), (odd, p2)):
            tile = src[b * 2 * C : (b + 1) * 2 * C, :]
            up = tile.astype(F32)
            for wt in range(3):
                val = tile if wt == 1 else moved(up, 1 - wt, W).astype(BF)
                at = pl.multiple_of((wt * 2 + d) * 2 * C, 2 * C)
                gg[pl.ds(at, 2 * C), b * W : b * W + W] = val
    both = dot_nt(gg[...], vv[...])
    span = 4 * C
    twos = []
    for wt in range(3):
        for ht in range(3):
            parts = []
            for d in range(2):
                at = (wt * 4 + d * 2) * C
                parts.append(
                    both[at : at + C, ht * span : ht * span + span]
                    + both[at + C : at + 2 * C, (ht + 1) * span : (ht + 2) * span]
                )
            twos.append(parts[0] + pltpu.roll(parts[1], span - C, 1))
    r2[...] = jnp.concatenate(dense(twos, C), axis=1)
    quarter = low // 2
    ps[...] = jnp.zeros(ps.shape, BF)
    for b in range(low // 2):
        for q in range(2):
            h = 2 * b + q
            at, lane = H * C + (h % quarter) * C, (h // quarter) * wide
            tile = p1[at : at + C, lane : lane + wide]
            up = tile.astype(F32)
            for wt in range(3):
                val = tile if wt == 1 else moved(up, wt - 1, wide).astype(BF)
                to = (q * 4 + wt) * C
                ps[to : to + C, b * wide : b * wide + wide] = val
    p3 = dot_nt(cc[...], ps[...])
    tiles = []
    for dt in range(3):
        for ht in range(3):
            first = ((2 - dt) * 4 + 2 - ht) * F
            second = first + F
            tiles.append(p3[first : first + F, :span] + p3[second : second + F, span:])
    tiles = dense(tiles, C)
    each, bits = F // count, count.bit_length() - 1
    row, col = iota((F, F), 0), iota((F, F), 1)
    chunk = row // each
    lowest, index = (chunk >> (bits - 1)) & 1, jnp.zeros((F, F), jnp.int32)
    for bit in range(1, bits):
        value = (chunk >> (bits - 1 - bit)) & 1
        lowest, index = lowest ^ value, index + (value << bit)
    order = (col == (index + lowest) * each + row % each).astype(F32).astype(BF)
    r3[...] = dot(order, jnp.concatenate(tiles, axis=1).astype(BF))
    first, own = 0, lax.axis_index("gx")
    for bit in range(bits):
        first = first ^ ((own >> bit) & 1)
    start = 0
    for src, half in ((r2, C // 2), (r3, F // 2)):
        for q in range(len(tiles)):
            lanes = slice(q * span, q * span + span)
            give = src[pl.ds(pl.multiple_of((1 - first) * half, half), half), lanes]
            packet[q, start : start + half, :] = give.astype(BF)
            keep[q, start : start + half, :] = src[pl.ds(pl.multiple_of(first * half, half), half), lanes]
        start += half


def dense(tiles, C):
    lane = iota(tiles[0].shape, 1)
    out = [None] * (-(-len(tiles) * 3 // 4))
    for q, tile in enumerate(tiles):
        first, offset = divmod(3 * q, 4)
        tile = jnp.where(lane < 3 * C, tile, 0.0)
        if offset:
            tile = pltpu.roll(tile, offset * C, 1)
        low = tile if offset < 2 else jnp.where(lane >= offset * C, tile, 0.0)
        out[first] = low if out[first] is None else out[first] + low
        if offset > 1:
            out[first + 1] = jnp.where(lane < offset * C, tile, 0.0)
    return out


def finish_kernel(C, count, own_half, got_half, part, two, three):
    span, half = 4 * C, C // 2
    first, own = 0, lax.axis_index("gx")
    for bit in range(count.bit_length() - 1):
        first = first ^ ((own >> bit) & 1)
    for t in range(27):
        dt, ht, wt = t // 9, t // 3 % 3, t % 3
        q, group = divmod(wt * 9 + ht * 3 + dt, 4)
        for src, at in ((own_half, first), (got_half, 1 - first)):
            tile = src[q]
            if group:
                tile = pltpu.roll(tile, span - group * C, 1)
            two[t, pl.ds(pl.multiple_of(at * half, half), half), :] = tile[:, :C]
        q, group = divmod(t, 4)
        tile = part[q]
        if group:
            tile = pltpu.roll(tile, span - group * C, 1)
        three[t] = tile[:, :C]


def backward_plane(C, H, W, kb, d, gw, zf):
    for b in range(H // 2):
        out = taps_sum(dot(kb[d], gw[:, b * W : b * W + W]), 2 * C, W)
        for q in range(2):
            for half in range(W // LANES):
                lanes = slice(half * LANES, (half + 1) * LANES)
                zf[half, pl.ds(2 * b + q, C, stride=H), :] = out[q * C : q * C + C, lanes]


def back_near_kernel(C, F, H, W, b1, p1, p2, kb, plane_near, gw, zf):
    low, halves = H // 2, W // LANES
    odd = parity()
    for src, plane in ((p1, 2 - odd), (p2, 1 + odd), (b1, 3 - 3 * odd)):
        fill_plane(gw, lambda h: src[h * C : h * C + C, :], H, low, 4, plane, C, W)
    zero = jnp.zeros((C, W), BF)
    fill_plane(gw, lambda h: zero, H, low, 4, 3 * odd, C, W)
    clear_ends(gw, 4, C, low, W)
    backward_plane(C, H, W, kb, 1 - odd, gw, zf)
    for half in range(halves):
        plane_near[:, half * LANES : (half + 1) * LANES] = zf[half].astype(BF)


def back_far_kernel(C, F, H, W, b1, b2, p1, kb, k3f, plane_near, gw_in, gv, ft, gw, pp, zf, ff):
    low, wide = H // 2, W // 2
    quarter, halves, low_halves = low // 2, W // LANES, wide // LANES
    odd = parity()
    scale = inside().astype(BF)
    fill_plane(gw, lambda h: b2[h * C : h * C + C, :] * scale, H, low, 4, 3 * odd, C, W)
    backward_plane(C, H, W, kb, odd, gw, zf)
    for c in range(C):
        rows = slice(c * H, c * H + H)
        gv[c, 1 - odd] = plane_near[rows, :]
        gv[c, odd] = jnp.concatenate([zf[half, rows, :] for half in range(halves)], axis=1).astype(BF)
    pp[...] = jnp.zeros(pp.shape, BF)
    for src, plane in ((b1, 2 - 2 * odd), (b2, 2 * odd), (p1, 1)):

        def tile_of(h):
            at, lane = H * C + (h % quarter) * C, (h // quarter) * wide
            tile = src[at : at + C, lane : lane + wide]
            return tile * scale if src is b2 else tile

        fill_plane(pp, tile_of, low, quarter, 4, plane, C, wide)
    out = taps_sum(dot(k3f[...], pp[...]), 2 * F, wide)
    for b in range(quarter):
        for q in range(2):
            for half in range(low_halves):
                lane = b * wide + half * LANES
                ff[half, pl.ds(2 * b + q, F, stride=low), :] = out[q * F : q * F + F, lane : lane + LANES]
    for half in range(low_halves):
        ft[:, half * LANES : (half + 1) * LANES] = ff[half].astype(BF)


def call(body, outs, scratch, flops, aliases, *args):
    return pl.pallas_call(
        body,
        out_shape=outs,
        in_specs=[VMEM] * len(args),
        out_specs=jax.tree.map(lambda _: VMEM, outs),
        scratch_shapes=scratch,
        cost_estimate=pl.CostEstimate(flops=flops // 1000, bytes_accessed=1024, transcendentals=0),
        compiler_params=pltpu.CompilerParams(vmem_limit_bytes=12 * 2**20),
        input_output_aliases=aliases,
    )(*args)


def swap(near, far, axis):
    count = lax.axis_size(axis)
    groups = lax.axis_size("groups")
    pairs = [(i, i + 1) for i in range(1, count - 1, 2)]
    pairs = [(g * count + a, g * count + b) for g in range(groups) for a, b in pairs]
    pairs += [(g * count + e, (g + 1) * count + e) for g in range(0, groups - 1, 2) for e in (0, count - 1)]
    got_far = lax.ppermute(far, ("groups", axis), pairs + [(b, a) for a, b in pairs])
    pairs = [(i, i + 1) for i in range(0, count - 1, 2)]
    got_near = lax.ppermute(near, axis, pairs + [(b, a) for a, b in pairs])
    return got_near, got_far


def reduce_both(packet, keep, shared, axis):
    count = lax.axis_size(axis)
    index = lax.axis_index(axis)
    exchange = lambda v, mask: lax.ppermute(v, axis, [(i, i ^ mask) for i in range(count)])
    keep = keep + exchange(packet, 1).astype(F32)
    full, part = keep[:, :shared], keep[:, shared:]
    step = 2
    while step < count:
        half = part.shape[1] // 2
        bit = (index // step) % 2
        give = lax.dynamic_slice_in_dim(part, (1 - bit) * half, half, 1).astype(BF)
        part = lax.dynamic_slice_in_dim(part, bit * half, half, 1)
        full = full.astype(BF)
        got = exchange(jnp.concatenate([full, give], axis=1), step | 1)
        full = full.astype(F32) + got[:, :shared].astype(F32)
        part = part + got[:, shared:].astype(F32)
        step *= 2
    other = exchange(full, 1)
    return full, other, part


def program(volume, weight_two, weight_three, cotangent):
    C, planes, H, W = volume.shape
    F, _, low, wide = cotangent.shape
    count = lax.axis_size("gx")
    assert planes == 2 and 2 * low == H and 2 * wide == W
    assert count > 1 and count & (count - 1) == 0 and F % count == 0
    sds = jax.ShapeDtypeStruct
    odd = lax.axis_index("gx") % 2
    w2 = jnp.transpose(weight_two, (2, 3, 4, 0, 1)).reshape(27, C, C)
    w3 = jnp.transpose(weight_three, (2, 3, 4, 1, 0)).reshape(27, C, F)
    cot = cotangent.reshape(F * low, wide)
    near = lax.dynamic_index_in_dim(volume, 1 - odd, 1, keepdims=False).reshape(C * H, W)
    far = lax.dynamic_index_in_dim(volume, odd, 1, keepdims=False).reshape(C * H, W)
    a1, a2 = swap(near, far, "gx")
    halves, low_halves = W // LANES, wide // LANES
    bind = lambda body: functools.partial(body, C, F, H, W)
    window, window_cot = sds((16 * C, low * W), BF), sds((12 * F, low // 2 * wide), BF)
    filters, slopes = sds((2, 6 * C, 16 * C), BF), sds((low, 2 * C, W), F32)
    plane_f32 = pltpu.VMEM((halves, C * H, LANES), F32)
    plane_low_f32 = pltpu.VMEM((low_halves, F * low, LANES), F32)
    ka, vv, slope_near, means = call(
        bind(near_kernel),
        (filters, window, slopes, sds((low, C, wide), F32)),
        [plane_f32],
        900_000_000,
        {},
        w2,
        near,
        far,
        a1,
    )
    c1, c2 = swap(cot, cot, "gx")
    kb, k3f, k3b, cc = call(
        bind(prep_kernel),
        (filters, sds((6 * F, 16 * C), BF), sds((6 * C, 12 * F), BF), window_cot),
        [plane_low_f32],
        400_000_000,
        {},
        w2,
        w3,
        cot,
    )
    rows = low // 2 * C
    slope_far, pooled, vv = call(
        bind(far_kernel),
        (slopes, sds((rows, W), BF), window),
        [plane_f32],
        700_000_000,
        {3: 2},
        a2,
        ka,
        means,
        vv,
    )
    rows = H * C + rows
    p1, p2, cc = call(
        bind(slope_kernel),
        (sds((rows, W), BF), sds((rows, W), BF), window_cot),
        [plane_low_f32, pltpu.VMEM((2 * C, low // 2 * wide), BF)],
        400_000_000,
        {6: 2},
        c1,
        c2,
        slope_near,
        slope_far,
        pooled,
        k3b,
        cc,
    )
    b1, b2 = swap(p1, p2, "gx")
    tiles, shared = 7, C // 2
    packet, keep = call(
        lambda *refs: grads_kernel(C, F, H, W, count, *refs),
        (sds((tiles, shared + F // 2, 4 * C), BF), sds((tiles, shared + F // 2, 4 * C), F32)),
        [
            pltpu.VMEM((12 * C, low * W), BF),
            pltpu.VMEM((8 * C, low // 2 * wide), BF),
            pltpu.VMEM((C, tiles * 4 * C), F32),
            pltpu.VMEM((F, tiles * 4 * C), F32),
        ],
        1_200_000_000,
        {},
        p1,
        p2,
        vv,
        cc,
    )
    full, other, part = reduce_both(packet, keep, shared, "gx")
    plane_near, gw = call(
        bind(back_near_kernel),
        (sds((C * H, W), BF), window),
        [plane_f32],
        500_000_000,
        {},
        b1,
        p1,
        p2,
        kb,
    )
    gv, ft, _ = call(
        bind(back_far_kernel),
        (sds((C, 2, H, W), BF), sds((F * low, wide), BF), window),
        [pltpu.VMEM((16 * C, low // 2 * wide), BF), plane_f32, plane_low_f32],
        700_000_000,
        {6: 2},
        b1,
        b2,
        p1,
        kb,
        k3f,
        plane_near,
        gw,
    )
    two, three = call(
        lambda *refs: finish_kernel(C, count, *refs),
        (sds((27, C, C), F32), sds((27, F // count, C), F32)),
        [],
        100_000,
        {},
        full,
        other,
        part,
    )
    unfold = lambda v: jnp.transpose(v.reshape(3, 3, 3, v.shape[1], C), (3, 4, 0, 1, 2))
    return (
        ft.reshape(F, 1, low, wide),
        unfold(three),
        unfold(two),
        gv,
    )


def solution(mesh):
    return jax.shard_map(
        program,
        mesh=mesh,
        in_specs=(
            P(None, ("groups", "gx"), None, None),
            P(),
            P(),
            P(None, ("groups", "gx"), None, None),
        ),
        out_specs=(
            P(None, ("groups", "gx"), None, None),
            P(("groups", "gx"), None, None, None, None),
            P("groups", None, None, None, None),
            P(None, ("groups", "gx"), None, None),
        ),
        check_vma=False,
    )
```

```python
import functools

import jax
import jax.numpy as jnp
from jax import lax
from jax.experimental import pallas as pl
from jax.experimental.pallas import tpu as pltpu
from jax.sharding import PartitionSpec as P


BF = jnp.bfloat16
F32 = jnp.float32
LANES = 128
VMEM = pl.BlockSpec(memory_space=pltpu.VMEM)


def dot(a, b):
    return jnp.dot(a, b, preferred_element_type=F32)


def dot_nt(a, b):
    return lax.dot_general(a, b, (((1,), (1,)), ((), ())), preferred_element_type=F32)


def iota(shape, dim):
    return lax.broadcasted_iota(jnp.int32, shape, dim)


def place(rows, lanes, offset):
    return (iota((rows, lanes), 1) == iota((rows, lanes), 0) + offset).astype(F32).astype(BF)


def moved(x, step, width):
    lanes = x.shape[1]
    w = iota(x.shape, 1) % width
    rolled = pltpu.roll(x, (-step) % lanes, 1)
    edge = width - 1 if step > 0 else 0
    return jnp.where(w == edge, 0.0, rolled)


def taps_sum(y, rows, width):
    return y[rows : 2 * rows] + moved(y[:rows], -1, width) + moved(y[2 * rows :], 1, width)


def tap(d, h, w):
    return d * 9 + h * 3 + w


def unpack(src_ref, f_ref, halves, scale=None):
    for half in range(halves):
        part = src_ref[:, half * LANES : (half + 1) * LANES].astype(F32)
        f_ref[half] = part if scale is None else part * scale


def row_of(f_ref, start, count, stride, first, last):
    parts = [f_ref[half, pl.ds(start, count, stride=stride), :] for half in range(first, last)]
    whole = parts[0] if len(parts) == 1 else jnp.concatenate(parts, axis=1)
    return whole.astype(BF)


def windows(h, pairs):
    return [(b, h + 1 - 2 * b) for b in range(pairs) if 0 <= h + 1 - 2 * b < 4]


def parity():
    return lax.axis_index("gx") % 2


def inside():
    index = lax.axis_index("gx")
    return jnp.where((index == 0) | (index == lax.axis_size("gx") - 1), 0.0, 1.0)


def fill_plane(dst, tile_of, rows, pairs, planes, plane, height, width):
    for h in range(rows):
        tile = tile_of(h)
        for b, j in windows(h, pairs):
            at = pl.multiple_of((j * planes + plane) * height, height)
            dst[pl.ds(at, height), b * width : b * width + width] = tile


def clear_ends(dst, planes, height, pairs, width):
    dst[: planes * height, :width] = jnp.zeros((planes * height, width), BF)
    dst[3 * planes * height :, (pairs - 1) * width :] = jnp.zeros((planes * height, width), BF)


def setup_kernel(C, F, H, W, w2, near, far, ka, vv, xf):
    span = 4 * C
    halves, low = W // LANES, H // 2
    odd = parity()
    ka[...] = jnp.zeros(ka.shape, BF)
    stacks = [w2[dt * 9 : dt * 9 + 9].reshape(9 * C, C) for dt in range(3)]
    for d in range(2):
        tiles = sum(dot(stacks[dt], place(C, span, (dt + d) * C)) for dt in range(3)).astype(BF)
        for wt in range(3):
            for h in range(2):
                at = (wt * 2 + h) * C
                for ht in range(3):
                    lane = (h + ht) * span
                    g = ht * 3 + wt
                    ka[d, at : at + C, lane : lane + span] = tiles[g * C : g * C + C]
    for src, plane in ((near, 2 - odd), (far, 1 + odd)):
        unpack(src, xf, halves)
        fill_plane(vv, lambda h: row_of(xf, h, C, H, 0, halves), H, low, 4, plane, C, W)
    zero = jnp.zeros((C, W), BF)
    fill_plane(vv, lambda h: zero, H, low, 4, 3 * odd, C, W)
    clear_ends(vv, 4, C, low, W)


def near_kernel(C, F, H, W, a1, ka, vv_in, slope, means, vv, xf):
    halves, low = W // LANES, H // 2
    odd = parity()
    unpack(a1, xf, halves)
    fill_plane(vv, lambda h: row_of(xf, h, C, H, 0, halves), H, low, 4, 3 - 3 * odd, C, W)
    forward_plane(C, H, W, ka, 1 - odd, vv, slope, lambda b, mean: means.__setitem__(b, mean))


def forward_plane(C, H, W, ka, d, vv, slope, put):
    wide = W // 2
    eighth = jnp.where(iota((W, wide), 0) // 2 == iota((W, wide), 1), 0.125, 0.0).astype(BF)
    for b in range(H // 2):
        value = taps_sum(dot(ka[d], vv[:, b * W : b * W + W]), 2 * C, W)
        sigma = jax.nn.sigmoid(value)
        slope[b] = sigma * (1.0 + value * (1.0 - sigma))
        sums = dot((value * sigma).astype(BF), eighth)
        put(b, sums[:C] + sums[C:])


def far_kernel(C, F, H, W, a2, ka, means, vv_in, slope, pooled, vv, xf):
    halves, low, wide = W // LANES, H // 2, W // 2
    odd = parity()
    unpack(a2, xf, halves, inside())
    fill_plane(vv, lambda h: row_of(xf, h, C, H, 0, halves), H, low, 4, 3 * odd, C, W)
    quarter = low // 2

    def put(b, mean):
        at, lane = (b % quarter) * C, (b // quarter) * wide
        pooled[at : at + C, lane : lane + wide] = (mean + means[b]).astype(BF)

    forward_plane(C, H, W, ka, odd, vv, slope, put)


def prep_kernel(C, F, H, W, w2, w3, cot, kb, k3f, k3b, cc, cf):
    span, low, wide = 4 * C, H // 2, W // 2
    kb[...] = jnp.zeros(kb.shape, BF)
    k3f[...] = jnp.zeros(k3f.shape, BF)
    eye_c = place(C, C, 0)
    zero_c = jnp.zeros((C, C), BF)
    for d in range(2):
        rows = []
        for wt in range(3):
            for ht in range(3):
                three = [w2[tap(2 - dt, 2 - ht, 2 - wt)] for dt in range(3)]
                rows += ([zero_c] + three) if d else (three + [zero_c])
        tiles = dot_nt(eye_c, jnp.concatenate(rows, axis=0)).astype(BF)
        for wt in range(3):
            for h in range(2):
                at = (wt * 2 + h) * C
                for ht in range(3):
                    lane = (h + ht) * span
                    q = wt * 3 + ht
                    kb[d, at : at + C, lane : lane + span] = tiles[:, q * span : q * span + span]
    zero_f = jnp.zeros((C, F), BF)
    rows = []
    for wt in range(3):
        for ht in range(3):
            rows += [w3[tap(dt, ht, wt)] for dt in range(3)] + [zero_f]
    tiles = dot_nt(place(F, F, 0), jnp.concatenate(rows, axis=0)).astype(BF)
    for wt in range(3):
        for h in range(2):
            at = (wt * 2 + h) * F
            for ht in range(3):
                lane = (h + ht) * span
                q = wt * 3 + ht
                k3f[at : at + F, lane : lane + span] = tiles[:, q * span : q * span + span]
    four = 4 * F
    picked = [
        jnp.concatenate([w3[tap(2 - dt, 2 - ht, 2 - wt)] for wt in range(3) for dt in range(3)], axis=0)
        for ht in range(3)
    ]
    for h in range(2):
        tiles = sum(dot(picked[ht], place(F, four, (ht + h) * F)) for ht in range(3)).astype(BF)
        for wt in range(3):
            at = (wt * 2 + h) * C
            for dt in range(3):
                q = wt * 3 + dt
                k3b[at : at + C, dt * four : dt * four + four] = tiles[q * C : q * C + C]
    unpack(cot, cf, wide // LANES)
    fill_cot(F, H, W, cc, cf, 1)
    for plane in range(3):
        cc[plane * four : plane * four + F, :wide] = jnp.zeros((F, wide), BF)
        cc[plane * four + 3 * F : plane * four + four, (low // 2 - 1) * wide :] = jnp.zeros((F, wide), BF)


def fill_cot(F, H, W, cc, cf, plane):
    low, wide = H // 2, W // 2
    for h in range(low):
        tile = row_of(cf, h, F, low, 0, wide // LANES)
        for b, j in windows(h, low // 2):
            at = pl.multiple_of((plane * 4 + j) * F, F)
            cc[pl.ds(at, F), b * wide : b * wide + wide] = tile


def slope_kernel(C, F, H, W, c1, c2, slope_near, slope_far, pooled, k3b, cc_in, p1, p2, cc, cf, bp):
    low, wide = H // 2, W // 2
    odd = parity()
    for src, plane, scale in ((c1, 2 - 2 * odd, None), (c2, 2 * odd, inside())):
        unpack(src, cf, wide // LANES, scale)
        fill_cot(F, H, W, cc, cf, plane)
    bp[...] = taps_sum(dot(k3b[...], cc[...]), 2 * C, wide).astype(BF)
    spread = jnp.where(iota((wide, W), 1) // 2 == iota((wide, W), 0), 0.125, 0.0).astype(BF)
    for b in range(low):
        back = dot(bp[(b % 2) * C : (b % 2) * C + C, (b // 2) * wide : (b // 2) * wide + wide], spread)
        back = jnp.concatenate([back, back], axis=0)
        for out, slope in ((p1, slope_near), (p2, slope_far)):
            out[b * 2 * C : (b + 1) * 2 * C, :] = (back * slope[b]).astype(BF)
    for out in (p1, p2):
        out[H * C :, :] = pooled[...]


def grads_kernel(C, F, H, W, count, p1, p2, vv, cc, packet, keep, gg, ps, r2, r3):
    low, wide = H // 2, W // 2
    odd = parity()
    for b in range(low):
        for d, src in ((1 - odd, p1), (odd, p2)):
            tile = src[b * 2 * C : (b + 1) * 2 * C, :]
            up = tile.astype(F32)
            for wt in range(3):
                val = tile if wt == 1 else moved(up, 1 - wt, W).astype(BF)
                at = pl.multiple_of((wt * 2 + d) * 2 * C, 2 * C)
                gg[pl.ds(at, 2 * C), b * W : b * W + W] = val
    both = dot_nt(gg[...], vv[...])
    span = 4 * C
    twos = []
    for wt in range(3):
        for ht in range(3):
            parts = []
            for d in range(2):
                at = (wt * 4 + d * 2) * C
                parts.append(
                    both[at : at + C, ht * span : ht * span + span]
                    + both[at + C : at + 2 * C, (ht + 1) * span : (ht + 2) * span]
                )
            twos.append(parts[0] + pltpu.roll(parts[1], span - C, 1))
    r2[...] = jnp.concatenate(dense(twos, C), axis=1)
    quarter = low // 2
    ps[...] = jnp.zeros(ps.shape, BF)
    for b in range(low // 2):
        for q in range(2):
            h = 2 * b + q
            at, lane = H * C + (h % quarter) * C, (h // quarter) * wide
            tile = p1[at : at + C, lane : lane + wide]
            up = tile.astype(F32)
            for wt in range(3):
                val = tile if wt == 1 else moved(up, wt - 1, wide).astype(BF)
                to = (q * 4 + wt) * C
                ps[to : to + C, b * wide : b * wide + wide] = val
    p3 = dot_nt(cc[...], ps[...])
    tiles = []
    for dt in range(3):
        for ht in range(3):
            first = ((2 - dt) * 4 + 2 - ht) * F
            second = first + F
            tiles.append(p3[first : first + F, :span] + p3[second : second + F, span:])
    tiles = dense(tiles, C)
    each, bits = F // count, count.bit_length() - 1
    row, col = iota((F, F), 0), iota((F, F), 1)
    chunk = row // each
    lowest, index = (chunk >> (bits - 1)) & 1, jnp.zeros((F, F), jnp.int32)
    for place_of, bit in enumerate(step_bits(count)):
        value = (chunk >> (bits - 2 - place_of)) & 1
        lowest, index = lowest ^ value, index + (value << bit)
    order = (col == (index + lowest) * each + row % each).astype(F32).astype(BF)
    r3[...] = dot(order, jnp.concatenate(tiles, axis=1).astype(BF))
    first, own = 0, lax.axis_index("gx")
    for bit in range(bits):
        first = first ^ ((own >> bit) & 1)
    start = 0
    for src, half in ((r2, C // 2), (r3, F // 2)):
        for q in range(len(tiles)):
            lanes = slice(q * span, q * span + span)
            give = src[pl.ds(pl.multiple_of((1 - first) * half, half), half), lanes]
            packet[q, start : start + half, :] = give.astype(BF)
            keep[q, start : start + half, :] = src[pl.ds(pl.multiple_of(first * half, half), half), lanes]
        start += half


def step_bits(count):
    bits = list(range(2, count.bit_length() - 1))
    return bits + [1] if count > 2 else bits


def dense(tiles, C):
    lane = iota(tiles[0].shape, 1)
    out = [None] * (-(-len(tiles) * 3 // 4))
    for q, tile in enumerate(tiles):
        first, offset = divmod(3 * q, 4)
        tile = jnp.where(lane < 3 * C, tile, 0.0)
        if offset:
            tile = pltpu.roll(tile, offset * C, 1)
        low = tile if offset < 2 else jnp.where(lane >= offset * C, tile, 0.0)
        out[first] = low if out[first] is None else out[first] + low
        if offset > 1:
            out[first + 1] = jnp.where(lane < offset * C, tile, 0.0)
    return out


def finish_kernel(C, count, own_half, got_half, part, two, three):
    span, half = 4 * C, C // 2
    first, own = 0, lax.axis_index("gx")
    for bit in range(count.bit_length() - 1):
        first = first ^ ((own >> bit) & 1)
    for t in range(27):
        dt, ht, wt = t // 9, t // 3 % 3, t % 3
        q, group = divmod(wt * 9 + ht * 3 + dt, 4)
        for src, at in ((own_half, first), (got_half, 1 - first)):
            tile = src[q]
            if group:
                tile = pltpu.roll(tile, span - group * C, 1)
            two[t, pl.ds(pl.multiple_of(at * half, half), half), :] = tile[:, :C]
        q, group = divmod(t, 4)
        tile = part[q]
        if group:
            tile = pltpu.roll(tile, span - group * C, 1)
        three[t] = tile[:, :C]


def backward_plane(C, H, W, kb, d, gw, zf):
    for b in range(H // 2):
        out = taps_sum(dot(kb[d], gw[:, b * W : b * W + W]), 2 * C, W)
        for q in range(2):
            for half in range(W // LANES):
                lanes = slice(half * LANES, (half + 1) * LANES)
                zf[half, pl.ds(2 * b + q, C, stride=H), :] = out[q * C : q * C + C, lanes]


def back_near_kernel(C, F, H, W, b1, p1, p2, kb, plane_near, gw, zf):
    low, halves = H // 2, W // LANES
    odd = parity()
    for src, plane in ((p1, 2 - odd), (p2, 1 + odd), (b1, 3 - 3 * odd)):
        fill_plane(gw, lambda h: src[h * C : h * C + C, :], H, low, 4, plane, C, W)
    zero = jnp.zeros((C, W), BF)
    fill_plane(gw, lambda h: zero, H, low, 4, 3 * odd, C, W)
    clear_ends(gw, 4, C, low, W)
    backward_plane(C, H, W, kb, 1 - odd, gw, zf)
    for half in range(halves):
        plane_near[:, half * LANES : (half + 1) * LANES] = zf[half].astype(BF)


def back_far_kernel(C, F, H, W, b1, b2, p1, p2, kb, k3f, plane_near, gv, ft, gw, pp, zf, ff):
    low, wide = H // 2, W // 2
    quarter, halves, low_halves = low // 2, W // LANES, wide // LANES
    odd = parity()
    scale = inside().astype(BF)
    for src, plane in ((p1, 2 - odd), (p2, 1 + odd), (b1, 3 - 3 * odd)):
        fill_plane(gw, lambda h: src[h * C : h * C + C, :], H, low, 4, plane, C, W)
    fill_plane(gw, lambda h: b2[h * C : h * C + C, :] * scale, H, low, 4, 3 * odd, C, W)
    clear_ends(gw, 4, C, low, W)
    backward_plane(C, H, W, kb, odd, gw, zf)
    for c in range(C):
        rows = slice(c * H, c * H + H)
        gv[c, 1 - odd] = plane_near[rows, :]
        gv[c, odd] = jnp.concatenate([zf[half, rows, :] for half in range(halves)], axis=1).astype(BF)
    pp[...] = jnp.zeros(pp.shape, BF)
    for src, plane in ((b1, 2 - 2 * odd), (b2, 2 * odd), (p1, 1)):

        def tile_of(h):
            at, lane = H * C + (h % quarter) * C, (h // quarter) * wide
            tile = src[at : at + C, lane : lane + wide]
            return tile * scale if src is b2 else tile

        fill_plane(pp, tile_of, low, quarter, 4, plane, C, wide)
    out = taps_sum(dot(k3f[...], pp[...]), 2 * F, wide)
    for b in range(quarter):
        for q in range(2):
            for half in range(low_halves):
                lane = b * wide + half * LANES
                ff[half, pl.ds(2 * b + q, F, stride=low), :] = out[q * F : q * F + F, lane : lane + LANES]
    for half in range(low_halves):
        ft[:, half * LANES : (half + 1) * LANES] = ff[half].astype(BF)


def call(body, outs, scratch, flops, aliases, *args):
    return pl.pallas_call(
        body,
        out_shape=outs,
        in_specs=[VMEM] * len(args),
        out_specs=jax.tree.map(lambda _: VMEM, outs),
        scratch_shapes=scratch,
        cost_estimate=pl.CostEstimate(flops=flops // 1000, bytes_accessed=1024, transcendentals=0),
        compiler_params=pltpu.CompilerParams(vmem_limit_bytes=12 * 2**20),
        input_output_aliases=aliases,
    )(*args)


def swap(near, far, axis):
    count = lax.axis_size(axis)
    groups = lax.axis_size("groups")
    pairs = [(i, i + 1) for i in range(1, count - 1, 2)]
    pairs = [(g * count + a, g * count + b) for g in range(groups) for a, b in pairs]
    pairs += [(g * count + e, (g + 1) * count + e) for g in range(0, groups - 1, 2) for e in (0, count - 1)]
    got_far = lax.ppermute(far, ("groups", axis), pairs + [(b, a) for a, b in pairs])
    pairs = [(i, i + 1) for i in range(0, count - 1, 2)]
    got_near = lax.ppermute(near, axis, pairs + [(b, a) for a, b in pairs])
    return got_near, got_far


def reduce_both(packet, keep, shared, axis):
    count = lax.axis_size(axis)
    index = lax.axis_index(axis)
    exchange = lambda v, mask: lax.ppermute(v, axis, [(i, i ^ mask) for i in range(count)])
    keep = keep + exchange(packet, 1).astype(F32)
    full, part = keep[:, :shared], keep[:, shared:]
    for bit in step_bits(count):
        half = part.shape[1] // 2
        own = (index >> bit) & 1
        give = lax.dynamic_slice_in_dim(part, (1 - own) * half, half, 1).astype(BF)
        part = lax.dynamic_slice_in_dim(part, own * half, half, 1)
        full = full.astype(BF)
        got = exchange(jnp.concatenate([full, give], axis=1), (1 << bit) | 1)
        full = full.astype(F32) + got[:, :shared].astype(F32)
        part = part + got[:, shared:].astype(F32)
    other = exchange(full, 1)
    return full, other, part


def program(volume, weight_two, weight_three, cotangent):
    C, planes, H, W = volume.shape
    F, _, low, wide = cotangent.shape
    count = lax.axis_size("gx")
    assert planes == 2 and 2 * low == H and 2 * wide == W
    assert count > 1 and count & (count - 1) == 0 and F % count == 0
    sds = jax.ShapeDtypeStruct
    odd = lax.axis_index("gx") % 2
    w2 = jnp.transpose(weight_two, (2, 3, 4, 0, 1)).reshape(27, C, C)
    w3 = jnp.transpose(weight_three, (2, 3, 4, 1, 0)).reshape(27, C, F)
    cot = cotangent.reshape(F * low, wide)
    near = lax.dynamic_index_in_dim(volume, 1 - odd, 1, keepdims=False).reshape(C * H, W)
    far = lax.dynamic_index_in_dim(volume, odd, 1, keepdims=False).reshape(C * H, W)
    a1, a2 = swap(near, far, "gx")
    halves, low_halves = W // LANES, wide // LANES
    bind = lambda body: functools.partial(body, C, F, H, W)
    window, window_cot = sds((16 * C, low * W), BF), sds((12 * F, low // 2 * wide), BF)
    filters, slopes = sds((2, 6 * C, 16 * C), BF), sds((low, 2 * C, W), F32)
    plane_f32 = pltpu.VMEM((halves, C * H, LANES), F32)
    plane_low_f32 = pltpu.VMEM((low_halves, F * low, LANES), F32)
    ka, vv = call(
        bind(setup_kernel), (filters, window), [plane_f32], 200_000_000, {}, w2, near, far
    )
    slope_near, means, vv = call(
        bind(near_kernel),
        (slopes, sds((low, C, wide), F32), window),
        [plane_f32],
        700_000_000,
        {2: 2},
        a1,
        ka,
        vv,
    )
    c1, c2 = swap(cot, cot, "gx")
    kb, k3f, k3b, cc = call(
        bind(prep_kernel),
        (filters, sds((6 * F, 16 * C), BF), sds((6 * C, 12 * F), BF), window_cot),
        [plane_low_f32],
        400_000_000,
        {},
        w2,
        w3,
        cot,
    )
    rows = low // 2 * C
    slope_far, pooled, vv = call(
        bind(far_kernel),
        (slopes, sds((rows, W), BF), window),
        [plane_f32],
        700_000_000,
        {3: 2},
        a2,
        ka,
        means,
        vv,
    )
    rows = H * C + rows
    p1, p2, cc = call(
        bind(slope_kernel),
        (sds((rows, W), BF), sds((rows, W), BF), window_cot),
        [plane_low_f32, pltpu.VMEM((2 * C, low // 2 * wide), BF)],
        400_000_000,
        {6: 2},
        c1,
        c2,
        slope_near,
        slope_far,
        pooled,
        k3b,
        cc,
    )
    b1, b2 = swap(p1, p2, "gx")
    tiles, shared = 7, C // 2
    packet, keep = call(
        lambda *refs: grads_kernel(C, F, H, W, count, *refs),
        (sds((tiles, shared + F // 2, 4 * C), BF), sds((tiles, shared + F // 2, 4 * C), F32)),
        [
            pltpu.VMEM((12 * C, low * W), BF),
            pltpu.VMEM((8 * C, low // 2 * wide), BF),
            pltpu.VMEM((C, tiles * 4 * C), F32),
            pltpu.VMEM((F, tiles * 4 * C), F32),
        ],
        1_200_000_000,
        {},
        p1,
        p2,
        vv,
        cc,
    )
    full, other, part = reduce_both(packet, keep, shared, "gx")
    plane_near = call(
        bind(back_near_kernel),
        sds((C * H, W), BF),
        [pltpu.VMEM(window.shape, BF), plane_f32],
        500_000_000,
        {},
        b1,
        p1,
        p2,
        kb,
    )
    gv, ft = call(
        bind(back_far_kernel),
        (sds((C, 2, H, W), BF), sds((F * low, wide), BF)),
        [pltpu.VMEM(window.shape, BF), pltpu.VMEM((16 * C, low // 2 * wide), BF), plane_f32, plane_low_f32],
        700_000_000,
        {},
        b1,
        b2,
        p1,
        p2,
        kb,
        k3f,
        plane_near,
    )
    two, three = call(
        lambda *refs: finish_kernel(C, count, *refs),
        (sds((27, C, C), F32), sds((27, F // count, C), F32)),
        [],
        100_000,
        {},
        full,
        other,
        part,
    )
    unfold = lambda v: jnp.transpose(v.reshape(3, 3, 3, v.shape[1], C), (3, 4, 0, 1, 2))
    return (
        ft.reshape(F, 1, low, wide),
        unfold(three),
        unfold(two),
        gv,
    )


def solution(mesh):
    return jax.shard_map(
        program,
        mesh=mesh,
        in_specs=(
            P(None, ("groups", "gx"), None, None),
            P(),
            P(),
            P(None, ("groups", "gx"), None, None),
        ),
        out_specs=(
            P(None, ("groups", "gx"), None, None),
            P(("groups", "gx"), None, None, None, None),
            P("groups", None, None, None, None),
            P(None, ("groups", "gx"), None, None),
        ),
        check_vma=False,
    )
```

```python
import functools

import jax
import jax.numpy as jnp
from jax import lax
from jax.experimental import pallas as pl
from jax.experimental.pallas import tpu as pltpu
from jax.sharding import PartitionSpec as P


BF = jnp.bfloat16
F32 = jnp.float32
LANES = 128
VMEM = pl.BlockSpec(memory_space=pltpu.VMEM)


def dot(a, b):
    return jnp.dot(a, b, preferred_element_type=F32)


def dot_nt(a, b):
    return lax.dot_general(a, b, (((1,), (1,)), ((), ())), preferred_element_type=F32)


def iota(shape, dim):
    return lax.broadcasted_iota(jnp.int32, shape, dim)


def place(rows, lanes, offset):
    return (iota((rows, lanes), 1) == iota((rows, lanes), 0) + offset).astype(F32).astype(BF)


def moved(x, step, width):
    lanes = x.shape[1]
    w = iota(x.shape, 1) % width
    rolled = pltpu.roll(x, (-step) % lanes, 1)
    edge = width - 1 if step > 0 else 0
    return jnp.where(w == edge, 0.0, rolled)


def taps_sum(y, rows, width):
    return y[rows : 2 * rows] + moved(y[:rows], -1, width) + moved(y[2 * rows :], 1, width)


def tap(d, h, w):
    return d * 9 + h * 3 + w


def unpack(src_ref, f_ref, halves, scale=None):
    for half in range(halves):
        part = src_ref[:, half * LANES : (half + 1) * LANES].astype(F32)
        f_ref[half] = part if scale is None else part * scale


def row_of(f_ref, start, count, stride, first, last):
    parts = [f_ref[half, pl.ds(start, count, stride=stride), :] for half in range(first, last)]
    whole = parts[0] if len(parts) == 1 else jnp.concatenate(parts, axis=1)
    return whole.astype(BF)


def windows(h, pairs):
    return [(b, h + 1 - 2 * b) for b in range(pairs) if 0 <= h + 1 - 2 * b < 4]


def parity():
    return lax.axis_index("gx") % 2


def inside():
    index = lax.axis_index("gx")
    return jnp.where((index == 0) | (index == lax.axis_size("gx") - 1), 0.0, 1.0)


def fill_plane(dst, tile_of, rows, pairs, plane, height, width):
    for h in range(rows):
        tile = tile_of(h)
        for b, j in windows(h, pairs):
            at = pl.multiple_of((plane * 4 + j) * height, height)
            dst[pl.ds(at, height), b * width : b * width + width] = tile


def clear_ends(dst, planes, height, pairs, width):
    for plane in range(planes):
        at = plane * 4 * height
        dst[at : at + height, :width] = jnp.zeros((height, width), BF)
        dst[at + 3 * height : at + 4 * height, (pairs - 1) * width :] = jnp.zeros((height, width), BF)


def setup_kernel(C, F, H, W, w2, near, far, ka, vv, xf):
    span = 4 * C
    halves, low = W // LANES, H // 2
    odd = parity()
    stacks = [
        jnp.concatenate([w2[tap(dt, ht, wt)] for dt in range(3) for wt in range(3)], axis=0) for ht in range(3)
    ]
    for h in range(2):
        tiles = sum(dot(stacks[ht], place(C, span, (ht + h) * C)) for ht in range(3)).astype(BF)
        for wt in range(3):
            at = (wt * 2 + h) * C
            for dt in range(3):
                g = dt * 3 + wt
                ka[at : at + C, dt * span : dt * span + span] = tiles[g * C : g * C + C]
    for src, plane in ((near, 2 - odd), (far, 1 + odd)):
        unpack(src, xf, halves)
        fill_plane(vv, lambda h: row_of(xf, h, C, H, 0, halves), H, low, plane, C, W)
    clear_ends(vv, 4, C, low, W)


def near_kernel(C, F, H, W, a1, ka, vv_in, slope, means, vv, xf, y):
    halves, low = W // LANES, H // 2
    odd = parity()
    unpack(a1, xf, halves)
    fill_plane(vv, lambda h: row_of(xf, h, C, H, 0, halves), H, low, 3 - 3 * odd, C, W)
    forward_plane(C, H, W, ka, 1 - odd, vv, y, slope, lambda b, mean: means.__setitem__(b, mean))


def overlapped(pairs, produce, consume):
    produce(0)
    for b in range(pairs):
        if b + 1 < pairs:
            produce(b + 1)
        consume(b)


def product(C, W, filters, d, window, y):
    start = pl.multiple_of(d * 4 * C, 4 * C)

    def produce(b):
        y[b] = dot(filters[...], window[pl.ds(start, 12 * C), b * W : b * W + W])

    return produce


def forward_plane(C, H, W, ka, d, vv, y, slope, put):
    wide = W // 2
    eighth = jnp.where(iota((W, wide), 0) // 2 == iota((W, wide), 1), 0.125, 0.0).astype(BF)

    def consume(b):
        value = taps_sum(y.at[b], 2 * C, W)
        sigma = jax.nn.sigmoid(value)
        slope[b] = sigma * (1.0 + value * (1.0 - sigma))
        sums = dot((value * sigma).astype(BF), eighth)
        put(b, sums[:C] + sums[C:])

    overlapped(H // 2, product(C, W, ka, d, vv, y), consume)


def far_kernel(C, F, H, W, a2, ka, means, vv_in, slope, pooled, vv, xf, y):
    halves, low, wide = W // LANES, H // 2, W // 2
    odd = parity()
    unpack(a2, xf, halves, inside())
    fill_plane(vv, lambda h: row_of(xf, h, C, H, 0, halves), H, low, 3 * odd, C, W)
    quarter = low // 2

    def put(b, mean):
        at, lane = (b % quarter) * C, (b // quarter) * wide
        pooled[at : at + C, lane : lane + wide] = (mean + means[b]).astype(BF)

    forward_plane(C, H, W, ka, odd, vv, y, slope, put)


def prep_kernel(C, F, H, W, w2, w3, cot, kb, k3f, k3b, cc, cf):
    span, low, wide = 4 * C, H // 2, W // 2
    fine = lambda dt, ht, wt: w2[tap(2 - dt, 2 - ht, 2 - wt)]
    coarse = lambda dt, ht, wt: w3[tap(dt, ht, wt)]
    for size, pick, out in ((C, fine, kb), (F, coarse, k3f)):
        zero = jnp.zeros((C, size), BF)
        for h in range(2):
            rows = []
            for wt in range(3):
                for dt in range(3):
                    three = [pick(dt, ht, wt) for ht in range(3)]
                    rows += ([zero] + three) if h else (three + [zero])
            tiles = dot_nt(place(size, size, 0), jnp.concatenate(rows, axis=0)).astype(BF)
            for wt in range(3):
                at = (wt * 2 + h) * size
                lane = wt * 3 * span
                out[at : at + size, :] = tiles[:, lane : lane + 3 * span]
    four = 4 * F
    picked = [
        jnp.concatenate([w3[tap(2 - dt, 2 - ht, 2 - wt)] for wt in range(3) for dt in range(3)], axis=0)
        for ht in range(3)
    ]
    for h in range(2):
        tiles = sum(dot(picked[ht], place(F, four, (ht + h) * F)) for ht in range(3)).astype(BF)
        for wt in range(3):
            at = (wt * 2 + h) * C
            for dt in range(3):
                q = wt * 3 + dt
                k3b[at : at + C, dt * four : dt * four + four] = tiles[q * C : q * C + C]
    unpack(cot, cf, wide // LANES)
    fill_cot(F, H, W, cc, cf, 1)
    clear_ends(cc, 3, F, low // 2, wide)


def fill_cot(F, H, W, cc, cf, plane):
    low, wide = H // 2, W // 2
    fill_plane(cc, lambda h: row_of(cf, h, F, low, 0, wide // LANES), low, low // 2, plane, F, wide)


def early_kernel(C, F, H, W, c1, pooled, cc_in, cc, ps, p3, cf):
    low, wide = H // 2, W // 2
    odd = parity()
    plane = 2 - 2 * odd
    unpack(c1, cf, wide // LANES)
    fill_cot(F, H, W, cc, cf, plane)
    quarter = low // 2
    ps[...] = jnp.zeros(ps.shape, BF)
    for b in range(low // 2):
        for q in range(2):
            h = 2 * b + q
            at, lane = (h % quarter) * C, (h // quarter) * wide
            tile = pooled[at : at + C, lane : lane + wide]
            up = tile.astype(F32)
            for wt in range(3):
                val = tile if wt == 1 else moved(up, wt - 1, wide).astype(BF)
                to = (q * 4 + wt) * C
                ps[to : to + C, b * wide : b * wide + wide] = val
    for at in (4 * F, pl.multiple_of(plane * 4 * F, 4 * F)):
        p3[pl.ds(at, 4 * F), :] = dot_nt(cc[pl.ds(at, 4 * F), :], ps[...])


def grads_kernel(C, F, H, W, count, *refs):
    c2, slope_near, slope_far, pooled, k3b, vv, ps, _, _ = refs[:9]
    p1, p2, packet, keep, cc, p3 = refs[9:15]
    cf, bp, gg, r2, r3 = refs[15:]
    low, wide, span = H // 2, W // 2, 4 * C
    odd = parity()
    plane = 2 * odd
    unpack(c2, cf, wide // LANES, inside())
    fill_cot(F, H, W, cc, cf, plane)
    bp[...] = taps_sum(dot(k3b[...], cc[...]), 2 * C, wide).astype(BF)
    at = pl.multiple_of(plane * 4 * F, 4 * F)
    p3[pl.ds(at, 4 * F), :] = dot_nt(cc[pl.ds(at, 4 * F), :], ps[...])
    spread = jnp.where(iota((wide, W), 1) // 2 == iota((wide, W), 0), 0.125, 0.0).astype(BF)
    for b in range(low):
        back = dot(bp[(b % 2) * C : (b % 2) * C + C, (b // 2) * wide : (b // 2) * wide + wide], spread)
        back = jnp.concatenate([back, back], axis=0)
        for d, out, slope in ((1 - odd, p1, slope_near), (odd, p2, slope_far)):
            tile = (back * slope[b]).astype(BF)
            out[b * 2 * C : (b + 1) * 2 * C, :] = tile
            up = tile.astype(F32)
            for wt in range(3):
                val = tile if wt == 1 else moved(up, 1 - wt, W).astype(BF)
                at = pl.multiple_of((d * 3 + wt) * 2 * C, 2 * C)
                gg[pl.ds(at, 2 * C), b * W : b * W + W] = val
    for out in (p1, p2):
        out[H * C :, :] = pooled[...]
    planes = [dot_nt(gg[d * 6 * C : (d + 1) * 6 * C, :], vv[d * span : d * span + 3 * span, :]) for d in range(2)]
    twos = []
    for wt in range(3):
        for dt in range(3):
            parts = []
            for h in range(2):
                at = (wt * 2 + h) * C
                parts.append(sum(both[at : at + C, dt * span : dt * span + span] for both in planes))
            twos.append(parts[0] + pltpu.roll(parts[1], span - C, 1))
    r2[...] = jnp.concatenate(dense(twos, C), axis=1)
    tiles = []
    for dt in range(3):
        for ht in range(3):
            first = ((2 - dt) * 4 + 2 - ht) * F
            second = first + F
            tiles.append(p3[first : first + F, :span] + p3[second : second + F, span:])
    tiles = dense(tiles, C)
    each, bits = F // count, count.bit_length() - 1
    row, col = iota((F, F), 0), iota((F, F), 1)
    chunk = row // each
    lowest, index = (chunk >> (bits - 1)) & 1, jnp.zeros((F, F), jnp.int32)
    for place_of, bit in enumerate(step_bits(count)):
        value = (chunk >> (bits - 2 - place_of)) & 1
        lowest, index = lowest ^ value, index + (value << bit)
    order = (col == (index + lowest) * each + row % each).astype(F32).astype(BF)
    r3[...] = dot(order, jnp.concatenate(tiles, axis=1).astype(BF))
    first, own = 0, lax.axis_index("gx")
    for bit in range(bits):
        first = first ^ ((own >> bit) & 1)
    start = 0
    for src, half in ((r2, C // 2), (r3, F // 2)):
        for q in range(len(tiles)):
            lanes = slice(q * span, q * span + span)
            give = src[pl.ds(pl.multiple_of((1 - first) * half, half), half), lanes]
            packet[q, start : start + half, :] = give.astype(BF)
            keep[q, start : start + half, :] = src[pl.ds(pl.multiple_of(first * half, half), half), lanes]
        start += half


def step_bits(count):
    bits = list(range(2, count.bit_length() - 1))
    return bits + [1] if count > 2 else bits


def dense(tiles, C):
    lane = iota(tiles[0].shape, 1)
    out = [None] * (-(-len(tiles) * 3 // 4))
    for q, tile in enumerate(tiles):
        first, offset = divmod(3 * q, 4)
        tile = jnp.where(lane < 3 * C, tile, 0.0)
        if offset:
            tile = pltpu.roll(tile, offset * C, 1)
        low = tile if offset < 2 else jnp.where(lane >= offset * C, tile, 0.0)
        out[first] = low if out[first] is None else out[first] + low
        if offset > 1:
            out[first + 1] = jnp.where(lane < offset * C, tile, 0.0)
    return out


def finish_kernel(C, count, own_half, got_half, part, two, three):
    span, half = 4 * C, C // 2
    first, own = 0, lax.axis_index("gx")
    for bit in range(count.bit_length() - 1):
        first = first ^ ((own >> bit) & 1)
    for t in range(27):
        dt, ht, wt = t // 9, t // 3 % 3, t % 3
        q, group = divmod(wt * 9 + dt * 3 + ht, 4)
        for src, at in ((own_half, first), (got_half, 1 - first)):
            tile = src[q]
            if group:
                tile = pltpu.roll(tile, span - group * C, 1)
            two[t, pl.ds(pl.multiple_of(at * half, half), half), :] = tile[:, :C]
        q, group = divmod(t, 4)
        tile = part[q]
        if group:
            tile = pltpu.roll(tile, span - group * C, 1)
        three[t] = tile[:, :C]


def backward_plane(C, H, W, kb, d, gw, y, zf):
    def consume(b):
        out = taps_sum(y.at[b], 2 * C, W)
        for q in range(2):
            for half in range(W // LANES):
                lanes = slice(half * LANES, (half + 1) * LANES)
                zf[half, pl.ds(2 * b + q, C, stride=H), :] = out[q * C : q * C + C, lanes]

    overlapped(H // 2, product(C, W, kb, d, gw, y), consume)


def back_near_kernel(C, F, H, W, b1, p1, p2, kb, plane_near, gw, zf, y):
    low, halves = H // 2, W // LANES
    odd = parity()
    for src, plane in ((p1, 2 - odd), (p2, 1 + odd), (b1, 3 - 3 * odd)):
        fill_plane(gw, lambda h: src[h * C : h * C + C, :], H, low, plane, C, W)
    clear_ends(gw, 4, C, low, W)
    backward_plane(C, H, W, kb, 1 - odd, gw, y, zf)
    for half in range(halves):
        plane_near[:, half * LANES : (half + 1) * LANES] = zf[half].astype(BF)


def back_far_kernel(C, F, H, W, b1, b2, p1, p2, kb, k3f, plane_near, gv, ft, gw, pp, zf, ff, y):
    low, wide = H // 2, W // 2
    quarter, halves, low_halves = low // 2, W // LANES, wide // LANES
    odd = parity()
    scale = inside().astype(BF)
    for src, plane in ((p1, 2 - odd), (p2, 1 + odd)):
        fill_plane(gw, lambda h: src[h * C : h * C + C, :], H, low, plane, C, W)
    fill_plane(gw, lambda h: b2[h * C : h * C + C, :] * scale, H, low, 3 * odd, C, W)
    clear_ends(gw, 4, C, low, W)
    backward_plane(C, H, W, kb, odd, gw, y, zf)
    for c in range(C):
        rows = slice(c * H, c * H + H)
        gv[c, 1 - odd] = plane_near[rows, :]
        gv[c, odd] = jnp.concatenate([zf[half, rows, :] for half in range(halves)], axis=1).astype(BF)
    clear_ends(pp, 3, C, quarter, wide)
    for src, plane in ((b1, 2 - 2 * odd), (b2, 2 * odd), (p1, 1)):

        def tile_of(h):
            at, lane = H * C + (h % quarter) * C, (h // quarter) * wide
            tile = src[at : at + C, lane : lane + wide]
            return tile * scale if src is b2 else tile

        fill_plane(pp, tile_of, low, quarter, plane, C, wide)
    out = taps_sum(dot(k3f[...], pp[...]), 2 * F, wide)
    for b in range(quarter):
        for q in range(2):
            for half in range(low_halves):
                lane = b * wide + half * LANES
                ff[half, pl.ds(2 * b + q, F, stride=low), :] = out[q * F : q * F + F, lane : lane + LANES]
    for half in range(low_halves):
        ft[:, half * LANES : (half + 1) * LANES] = ff[half].astype(BF)


def call(body, outs, scratch, flops, aliases, *args):
    return pl.pallas_call(
        body,
        out_shape=outs,
        in_specs=[VMEM] * len(args),
        out_specs=jax.tree.map(lambda _: VMEM, outs),
        scratch_shapes=scratch,
        cost_estimate=pl.CostEstimate(flops=flops // 1000, bytes_accessed=1024, transcendentals=0),
        compiler_params=pltpu.CompilerParams(vmem_limit_bytes=12 * 2**20),
        input_output_aliases=aliases,
    )(*args)


def swap(near, far, axis):
    count = lax.axis_size(axis)
    groups = lax.axis_size("groups")
    pairs = [(i, i + 1) for i in range(1, count - 1, 2)]
    pairs = [(g * count + a, g * count + b) for g in range(groups) for a, b in pairs]
    pairs += [(g * count + e, (g + 1) * count + e) for g in range(0, groups - 1, 2) for e in (0, count - 1)]
    got_far = lax.ppermute(far, ("groups", axis), pairs + [(b, a) for a, b in pairs])
    pairs = [(i, i + 1) for i in range(0, count - 1, 2)]
    got_near = lax.ppermute(near, axis, pairs + [(b, a) for a, b in pairs])
    return got_near, got_far


def reduce_both(packet, keep, shared, axis):
    count = lax.axis_size(axis)
    index = lax.axis_index(axis)
    exchange = lambda v, mask: lax.ppermute(v, axis, [(i, i ^ mask) for i in range(count)])
    keep = keep + exchange(packet, 1).astype(F32)
    full, part = keep[:, :shared], keep[:, shared:]
    for bit in step_bits(count):
        half = part.shape[1] // 2
        own = (index >> bit) & 1
        give = lax.dynamic_slice_in_dim(part, (1 - own) * half, half, 1).astype(BF)
        part = lax.dynamic_slice_in_dim(part, own * half, half, 1)
        full = full.astype(BF)
        got = exchange(jnp.concatenate([full, give], axis=1), (1 << bit) | 1)
        full = full.astype(F32) + got[:, :shared].astype(F32)
        part = part + got[:, shared:].astype(F32)
    other = exchange(full, 1)
    return full, other, part


def program(volume, weight_two, weight_three, cotangent):
    C, planes, H, W = volume.shape
    F, _, low, wide = cotangent.shape
    count = lax.axis_size("gx")
    assert planes == 2 and 2 * low == H and 2 * wide == W
    assert count > 1 and count & (count - 1) == 0 and F % count == 0
    sds = jax.ShapeDtypeStruct
    odd = lax.axis_index("gx") % 2
    w2 = jnp.transpose(weight_two, (2, 3, 4, 0, 1)).reshape(27, C, C)
    w3 = jnp.transpose(weight_three, (2, 3, 4, 1, 0)).reshape(27, C, F)
    cot = cotangent.reshape(F * low, wide)
    near = lax.dynamic_index_in_dim(volume, 1 - odd, 1, keepdims=False).reshape(C * H, W)
    far = lax.dynamic_index_in_dim(volume, odd, 1, keepdims=False).reshape(C * H, W)
    a1, a2 = swap(near, far, "gx")
    halves, low_halves = W // LANES, wide // LANES
    bind = lambda body: functools.partial(body, C, F, H, W)
    window, window_cot = sds((16 * C, low * W), BF), sds((12 * F, low // 2 * wide), BF)
    filters, slopes = sds((6 * C, 12 * C), BF), sds((low, 2 * C, W), F32)
    products = pltpu.VMEM((low, 6 * C, W), F32)
    plane_f32 = pltpu.VMEM((halves, C * H, LANES), F32)
    plane_low_f32 = pltpu.VMEM((low_halves, F * low, LANES), F32)
    ka, vv = call(
        bind(setup_kernel), (filters, window), [plane_f32], 200_000_000, {}, w2, near, far
    )
    slope_near, means, vv = call(
        bind(near_kernel),
        (slopes, sds((low, C, wide), F32), window),
        [plane_f32, products],
        700_000_000,
        {2: 2},
        a1,
        ka,
        vv,
    )
    c1, c2 = swap(cot, cot, "gx")
    kb, k3f, k3b, cc = call(
        bind(prep_kernel),
        (filters, sds((6 * F, 12 * C), BF), sds((6 * C, 12 * F), BF), window_cot),
        [plane_low_f32],
        400_000_000,
        {},
        w2,
        w3,
        cot,
    )
    rows = low // 2 * C
    slope_far, pooled, vv = call(
        bind(far_kernel),
        (slopes, sds((rows, W), BF), window),
        [plane_f32, products],
        700_000_000,
        {3: 2},
        a2,
        ka,
        means,
        vv,
    )
    tiles, shared = 7, C // 2
    shifted, partial = sds((8 * C, low // 2 * wide), BF), sds((12 * F, 8 * C), F32)
    cc, ps, p3 = call(
        bind(early_kernel),
        (window_cot, shifted, partial),
        [plane_low_f32],
        100_000_000,
        {2: 0},
        c1,
        pooled,
        cc,
    )
    rows = H * C + rows
    p1, p2, packet, keep, _, _ = call(
        lambda *refs: grads_kernel(C, F, H, W, count, *refs),
        (
            sds((rows, W), BF),
            sds((rows, W), BF),
            sds((tiles, shared + F // 2, 4 * C), BF),
            sds((tiles, shared + F // 2, 4 * C), F32),
            window_cot,
            partial,
        ),
        [
            plane_low_f32,
            pltpu.VMEM((2 * C, low // 2 * wide), BF),
            pltpu.VMEM((12 * C, low * W), BF),
            pltpu.VMEM((C, tiles * 4 * C), F32),
            pltpu.VMEM((F, tiles * 4 * C), F32),
        ],
        1_200_000_000,
        {7: 4, 8: 5},
        c2,
        slope_near,
        slope_far,
        pooled,
        k3b,
        vv,
        ps,
        cc,
        p3,
    )
    b1, b2 = swap(p1, p2, "gx")
    full, other, part = reduce_both(packet, keep, shared, "gx")
    plane_near = call(
        bind(back_near_kernel),
        sds((C * H, W), BF),
        [pltpu.VMEM(window.shape, BF), plane_f32, products],
        500_000_000,
        {},
        b1,
        p1,
        p2,
        kb,
    )
    gv, ft = call(
        bind(back_far_kernel),
        (sds((C, 2, H, W), BF), sds((F * low, wide), BF)),
        [pltpu.VMEM(window.shape, BF), pltpu.VMEM((12 * C, low // 2 * wide), BF), plane_f32, plane_low_f32, products],
        700_000_000,
        {},
        b1,
        b2,
        p1,
        p2,
        kb,
        k3f,
        plane_near,
    )
    two, three = call(
        lambda *refs: finish_kernel(C, count, *refs),
        (sds((27, C, C), F32), sds((27, F // count, C), F32)),
        [],
        100_000,
        {},
        full,
        other,
        part,
    )
    unfold = lambda v: jnp.transpose(v.reshape(3, 3, 3, v.shape[1], C), (3, 4, 0, 1, 2))
    return (
        ft.reshape(F, 1, low, wide),
        unfold(three),
        unfold(two),
        gv,
    )


def solution(mesh):
    return jax.shard_map(
        program,
        mesh=mesh,
        in_specs=(
            P(None, ("groups", "gx"), None, None),
            P(),
            P(),
            P(None, ("groups", "gx"), None, None),
        ),
        out_specs=(
            P(None, ("groups", "gx"), None, None),
            P(("groups", "gx"), None, None, None, None),
            P("groups", None, None, None, None),
            P(None, ("groups", "gx"), None, None),
        ),
        check_vma=False,
    )
```
